256 devices in a mesh: section: 2 (over core), tensor: 2 (over x_lo), dp: 64 (over z, y, x_hi).
Axes of the slice: x: 4 (x_hi: 2, x_lo: 2; x = x_hi * 2 + x_lo), y: 4, z: 8, core: 2. Of those that a mesh axis runs over, the one named last changes fastest.
Arguments:
- exit_hidden: bfloat16 [512, 4, 2048], P('dp', None, ('section', 'tensor')), may hold values from -6 to 6
- exit_depth: int32 [512], P('dp'), may hold values from 0 to 1, as said below
- context_len: int32 [512], P('dp'), may hold values from 48 to 384
- attn_gain: float32 [2, 2048], P('section'), may hold values from 0.1 to 1.9
- w_query: bfloat16 [2, 2048, 2048], P('section', None, 'tensor'), may hold values from -0.125 to 0.125
- w_keyval: bfloat16 [2, 2048, 1024], P('section', None, 'tensor'), may hold values from -0.125 to 0.125
- w_out: bfloat16 [2, 2048, 2048], P('section', 'tensor'), may hold values from -0.125 to 0.125
- kv_cache: bfloat16 [2, 512, 384, 8, 128], P('section', 'dp', None, 'tensor'), may hold values from -400 to 400
- mlp_gain: float32 [2, 2048], P('section'), may hold values from 0.1 to 1.9
- w_gate: bfloat16 [2, 2048, 4096], P('section', 'dp', 'tensor'), may hold values from -0.125 to 0.125
- w_up: bfloat16 [2, 2048, 4096], P('section', 'dp', 'tensor'), may hold values from -0.125 to 0.125
- w_down: bfloat16 [2, 2048, 4096], P('section', 'dp', 'tensor'), may hold values from -0.09375 to 0.09375
Outputs:
- layer_states: bfloat16 [2, 512, 4, 2048], P('section', 'dp', None, 'tensor')
The draws below stay inside these ranges and needn't reach their ends.
Inputs may be any that keep to these rules, and one draw needn't show every extreme that they name: `exit_depth`: every depth from 0 to 1 is held by some request.
All inputs are finite; a program needn't handle non-finite values.
Results may differ from the reference program's by a relative error of at most 0.019.
Values may be sent and summed in bfloat16 or wider, within the bound.
No kernel may reach another device: no remote copies, remote signals or barrier semaphores. Data moves between devices by JAX's collectives and lax.ppermute only.
A program may use at most 192 MiB of HBM per device.

```python
import math
import jax
import jax.numpy as jnp
from jax import lax

D = 2048
HEADS = 32
KV_HEADS = 8
HD = 64
FF = 4096
DRAFT = 4
CTX = 384
REQUESTS = 512
LAYERS = 2


def draw_exit_depth(key, part):
    first_key, second_key, order_key = jax.random.split(jax.random.fold_in(key, 11), 3)
    first = jax.random.randint(first_key, (REQUESTS,), 0, LAYERS)
    second = jax.random.randint(second_key, (REQUESTS,), 0, LAYERS)
    depth = jnp.minimum(first, second).astype(jnp.int32)
    order = jax.random.permutation(order_key, REQUESTS)
    depth = depth.at[order[:LAYERS]].set(jnp.arange(LAYERS, dtype=jnp.int32))
    return depth.astype(jnp.int32)


def draw_kv_cache(key, part):
    base = jax.random.normal(jax.random.fold_in(key, 21), (LAYERS, REQUESTS, CTX, KV_HEADS, 2 * HD), jnp.float32)
    return base.astype(jnp.bfloat16)


def with_ends(entries, stream_key, least, largest):
    longest = entries.shape.index(max(entries.shape))
    spots = []
    for shift in (0, 1):
        where = [jax.random.randint(jax.random.fold_in(stream_key, axis), (), 0, length) for axis, length in enumerate(entries.shape)]
        where[longest] = (where[longest] + shift) % entries.shape[longest]
        spots.append(tuple(where))
    return entries.at[spots[0]].set(least).at[spots[1]].set(largest)


def steps_of(key, dims, cuts, smallest, high):
    def one(dim, parts):
        heights = jax.random.uniform(jax.random.fold_in(jax.random.fold_in(key, 6), dim), (parts,), jnp.float32, smallest / len(cuts), high / len(cuts))
        return jnp.repeat(jnp.exp(heights), dims[dim] // parts).reshape((-1,) + (1,) * (len(dims) - dim - 1))

    level = one(*cuts[0])
    for cut in cuts[1:]:
        level = level * one(*cut)
    return level


def noise(key, dims, deviation, limit, shards=(), kind=jnp.bfloat16):
    result = deviation * jax.random.normal(key, dims, jnp.float32)
    if shards:
        result = result * steps_of(key, dims, shards, -0.22, 0.18)
    return jnp.clip(result, -limit, limit).astype(kind)


def setup_inputs(seed: int = 0) -> dict:
    streams_of = jax.random.split(jax.random.key(seed), 13)
    exit_hidden = noise(streams_of[0], (REQUESTS, DRAFT, D), 1.0, 6.0, ((0, 64), (2, 4)))
    exit_depth = draw_exit_depth(jax.random.fold_in(streams_of[12], 71), 0)
    context_len = with_ends(jax.random.randint(streams_of[2], (REQUESTS,), CTX // 8, CTX + 1), jax.random.fold_in(streams_of[2], 1), CTX // 8, CTX).astype(jnp.int32)
    attn_gain = jnp.clip(1.0 + 0.18 * jax.random.normal(streams_of[3], (LAYERS, D), jnp.float32), 0.1, 1.9)
    w_query = noise(streams_of[4], (LAYERS, D, HEADS * HD), D ** -0.5, 0.125, ((0, 2), (2, 2)))
    w_keyval = noise(streams_of[5], (LAYERS, D, KV_HEADS * 2 * HD), D ** -0.5, 0.125, ((0, 2), (2, 2)))
    w_out = noise(streams_of[6], (LAYERS, HEADS * HD, D), (HEADS * HD) ** -0.5, 0.125, ((0, 2), (1, 2)))
    kv_cache = draw_kv_cache(jax.random.fold_in(streams_of[12], 71), 0)
    mlp_gain = jnp.clip(1.0 + 0.18 * jax.random.normal(streams_of[8], (LAYERS, D), jnp.float32), 0.1, 1.9)
    w_gate = noise(streams_of[9], (LAYERS, D, FF), D ** -0.5, 0.125, ((0, 2), (1, 64), (2, 2)))
    w_up = noise(streams_of[10], (LAYERS, D, FF), D ** -0.5, 0.125, ((0, 2), (1, 64), (2, 2)))
    w_down = noise(streams_of[11], (LAYERS, D, FF), FF ** -0.5, 0.09375, ((0, 2), (1, 64), (2, 2)))
    return {"exit_hidden": exit_hidden, "exit_depth": exit_depth, "context_len": context_len, "attn_gain": attn_gain, "w_query": w_query, "w_keyval": w_keyval, "w_out": w_out, "kv_cache": kv_cache, "mlp_gain": mlp_gain, "w_gate": w_gate, "w_up": w_up, "w_down": w_down}


EPS = 1e-05
THETA = 500000.0
NEGATIVE = -1e+30

def rotate(values, where_at):
    middle = values.shape[-1] // 2
    rates = jnp.exp(jnp.arange(middle, dtype=jnp.float32) * (-2.0 * math.log(THETA) / values.shape[-1]))
    angles = where_at.astype(jnp.float32)[..., None] * rates
    cosine = jnp.cos(angles)
    sine = jnp.sin(angles)
    first = values[..., :middle]
    second = values[..., middle:]
    return jnp.concatenate([first * cosine - second * sine, second * cosine + first * sine], axis=-1)

def normalize(hidden, gain):
    wide = hidden.astype(jnp.float32)
    factor = lax.rsqrt(lax.optimization_barrier(jnp.mean(wide * wide, axis=-1, keepdims=True)) + EPS)
    return (wide * factor * gain).astype(jnp.bfloat16)

def attend(normed, lengths, cache, w_query, w_keyval, w_out):
    rows, drafts, width = normed.shape
    head_size = cache.shape[-1] // 2
    kv_count = cache.shape[2]
    q_count = w_query.shape[-1] // head_size
    group = q_count // kv_count
    flat = normed.reshape(rows * drafts, width)
    query = jnp.dot(flat, w_query, preferred_element_type=jnp.float32).reshape(rows, drafts, kv_count, group, head_size)
    keyval = jnp.dot(flat, w_keyval, preferred_element_type=jnp.float32).reshape(rows, drafts, kv_count, 2 * head_size)
    places = lengths[:, None] + jnp.arange(drafts, dtype=jnp.int32)[None, :]
    query = rotate(query, places[:, :, None, None]).astype(jnp.bfloat16)
    fresh_keys = rotate(keyval[..., :head_size], places[:, :, None]).astype(jnp.bfloat16)
    fresh_values = keyval[..., head_size:].astype(jnp.bfloat16)
    cached_keys = cache[..., :head_size].astype(jnp.float32)
    cached_values = cache[..., head_size:].astype(jnp.float32)
    scale = head_size ** (-0.5)
    query_wide = query.astype(jnp.float32)
    old_scores = jnp.einsum('rjkgd,rpkd->rkgjp', query_wide, cached_keys, precision=lax.Precision.HIGHEST) * scale
    live = jnp.arange(cache.shape[1], dtype=jnp.int32)[None, :] < lengths[:, None]
    old_scores = jnp.where(live[:, None, None, None, :], old_scores, NEGATIVE)
    new_scores = jnp.einsum('rjkgd,rikd->rkgji', query_wide, fresh_keys.astype(jnp.float32), precision=lax.Precision.HIGHEST) * scale
    causal = jnp.arange(drafts)[None, :] <= jnp.arange(drafts)[:, None]
    new_scores = jnp.where(causal, new_scores, NEGATIVE)
    top = jnp.maximum(old_scores.max(axis=-1), new_scores.max(axis=-1))[..., None]
    old_weights = jnp.exp(old_scores - top)
    new_weights = jnp.exp(new_scores - top)
    total = old_weights.sum(axis=-1, keepdims=True) + new_weights.sum(axis=-1, keepdims=True)
    old_weights = (old_weights / total).astype(jnp.bfloat16).astype(jnp.float32)
    new_weights = (new_weights / total).astype(jnp.bfloat16).astype(jnp.float32)
    mixed = jnp.einsum('rkgjp,rpkd->rjkgd', old_weights, cached_values, precision=lax.Precision.HIGHEST)
    mixed = mixed + jnp.einsum('rkgji,rikd->rjkgd', new_weights, fresh_values.astype(jnp.float32), precision=lax.Precision.HIGHEST)
    heads_out = mixed.astype(jnp.bfloat16).reshape(rows * drafts, q_count * head_size)
    return jnp.dot(heads_out, w_out, preferred_element_type=jnp.float32)

def feed_forward(normed, w_gate, w_up, w_down):
    flat = normed.reshape(-1, normed.shape[-1])
    gate = jnp.dot(flat, w_gate, preferred_element_type=jnp.float32)
    up = jnp.dot(flat, w_up, preferred_element_type=jnp.float32)
    act = (jax.nn.silu(gate) * up).astype(jnp.bfloat16)
    return jnp.dot(act, w_down.T, preferred_element_type=jnp.float32)

def reference(exit_hidden, exit_depth, context_len, attn_gain, w_query, w_keyval, w_out, kv_cache, mlp_gain, w_gate, w_up, w_down):
    current = exit_hidden
    states = []
    for layer in range(LAYERS):
        take = (exit_depth >= layer)[:, None, None]
        keep = (exit_depth <= layer)[:, None, None]
        whole = jnp.where(take, exit_hidden, current)
        partial_value = attend(normalize(whole, attn_gain[layer]), context_len, kv_cache[layer], w_query[layer], w_keyval[layer], w_out[layer])
        middle = (whole.astype(jnp.float32) + partial_value.reshape(whole.shape)).astype(jnp.bfloat16)
        branch = feed_forward(normalize(middle, mlp_gain[layer]), w_gate[layer], w_up[layer], w_down[layer])
        updated = (middle.astype(jnp.float32) + branch.reshape(whole.shape)).astype(jnp.bfloat16)
        current = jnp.where(keep, updated, whole)
        states.append(current)
    return jnp.stack(states)
```

```python
import math

import jax
import jax.numpy as jnp
from jax import lax
from jax.experimental import pallas as pl
from jax.experimental.pallas import tpu as pltpu
from jax.sharding import Mesh, PartitionSpec as P

D = 2048
DRAFT = 4
CTX = 384
ROWS = 8
TOKENS = ROWS * DRAFT
HD = 64
QH = 16
KH = 4
SLOTS = CTX * KH
VMEM_LIMIT = 60 * 1024 * 1024
FFS = 256
EPS = 1e-05
THETA = 500000.0
NEGATIVE = -1e30
PLANE = ("tensor", "y", "xh")
CHIP = ("section", "tensor")
Z = 8


def attend_kernel(
    lens, hidden, gain, cosine, sine, wq_h, wkv_h, wo_h, kv_h, out, wq, wkv, wo, kv, qs, nk, hs, bias, sems
):
    pieces = 4
    step = D // pieces
    copies = []
    for p in range(pieces):
        at = pl.ds(p * step, step)
        copies.append(pltpu.make_async_copy(wq_h.at[at], wq.at[at], sems.at[2 * p]))
        copies.append(pltpu.make_async_copy(wkv_h.at[at], wkv.at[at], sems.at[2 * p + 1]))
    base = 2 * pieces
    kv_copies = [
        pltpu.make_async_copy(kv_h.at[r], kv.at[r], sems.at[base + r]) for r in range(ROWS)
    ]
    wo_copy = pltpu.make_async_copy(wo_h, wo, sems.at[base + ROWS])
    for c in copies + kv_copies + [wo_copy]:
        c.start()

    row = lax.broadcasted_iota(jnp.int32, (4 * QH, SLOTS), 0)
    place = lax.broadcasted_iota(jnp.int32, (4 * QH, SLOTS), 1)
    bias[...] = jnp.where((place & 3) == (row >> 4), 0.0, NEGATIVE)
    new_row = lax.broadcasted_iota(jnp.int32, (4 * QH, DRAFT * KH), 0)
    new_col = lax.broadcasted_iota(jnp.int32, (4 * QH, DRAFT * KH), 1)
    seen = ((new_col & 3) == (new_row >> 4)) & ((new_col >> 2) <= (new_row & 3))

    wide = hidden[...].astype(jnp.float32)
    factor = lax.rsqrt(jnp.mean(wide * wide, axis=-1, keepdims=True) + EPS)
    normed = (wide * factor * gain[...]).astype(jnp.bfloat16)
    q = jnp.zeros((TOKENS, QH * HD), jnp.float32)
    new = jnp.zeros((TOKENS, KH * 2 * HD), jnp.float32)
    for p in range(pieces):
        at = pl.ds(p * step, step)
        copies[2 * p].wait()
        copies[2 * p + 1].wait()
        part = normed[:, p * step : (p + 1) * step]
        q = q + jnp.dot(part, wq[at], preferred_element_type=jnp.float32)
        new = new + jnp.dot(part, wkv[at], preferred_element_type=jnp.float32)

    lane = lax.broadcasted_iota(jnp.int32, (TOKENS, 128), 1)
    low = (lane & 63) < 32
    left = lane < HD
    cos_all = cosine[...]
    sin_all = sine[...]

    def turned(block, c, s):
        other = jnp.where(low, pltpu.roll(block, 96, 1), pltpu.roll(block, 32, 1))
        return block * c + other * s

    scale = HD ** (-0.5)
    for m in range(QH // 2):
        block = turned(q[:, m * 128 : (m + 1) * 128], cos_all, sin_all) * scale
        pair = (jnp.where(left, block, 0.0), jnp.where(left, pltpu.roll(block, HD, 1), 0.0))
        for half in range(2):
            for j in range(DRAFT):
                at = ((2 * m + half) * DRAFT + j) * ROWS
                qs[at : at + ROWS, :] = pair[half][j * ROWS : (j + 1) * ROWS, :]
    key_cos = jnp.where(left, cos_all, 1.0)
    key_sin = jnp.where(left, sin_all, 0.0)
    for h in range(KH):
        block = turned(new[:, h * 128 : (h + 1) * 128], key_cos, key_sin)
        for i in range(DRAFT):
            at = (i * KH + h) * ROWS
            nk[at : at + ROWS, :] = block[i * ROWS : (i + 1) * ROWS, :]

    last = (((1,), (1,)), ((), ()))
    for r in range(ROWS):
        fresh = nk[pl.ds(r, DRAFT * KH, stride=ROWS), :].astype(jnp.bfloat16)
        mine = qs[pl.ds(r, 4 * QH, stride=ROWS), :].astype(jnp.bfloat16)
        kv_copies[r].wait()
        stored = kv[r]
        scores = lax.dot_general(mine, stored, last, preferred_element_type=jnp.float32)
        scores = jnp.where(place < KH * lens[r], scores, NEGATIVE) + bias[...]
        new_scores = lax.dot_general(mine, fresh, last, preferred_element_type=jnp.float32)
        new_scores = jnp.where(seen, new_scores, NEGATIVE)
        top = jnp.maximum(
            jnp.max(scores, axis=-1, keepdims=True), jnp.max(new_scores, axis=-1, keepdims=True)
        )
        weights = jnp.exp(scores - top)
        new_weights = jnp.exp(new_scores - top)
        total = jnp.sum(weights, axis=-1, keepdims=True) + jnp.sum(
            new_weights, axis=-1, keepdims=True
        )
        mixed = jnp.dot(
            weights.astype(jnp.bfloat16), stored, preferred_element_type=jnp.float32
        ) + jnp.dot(new_weights.astype(jnp.bfloat16), fresh, preferred_element_type=jnp.float32)
        hs[pl.ds(r, 4 * QH, stride=ROWS), :] = mixed / total

    side = lax.broadcasted_iota(jnp.int32, (ROWS, 128), 1) < HD
    rows = []
    for j in range(DRAFT):
        tiles = []
        for m in range(QH // 2):
            first = ((2 * m) * DRAFT + j) * ROWS
            second = ((2 * m + 1) * DRAFT + j) * ROWS
            tiles.append(
                jnp.where(
                    side, pltpu.roll(hs[first : first + ROWS, :], HD, 1), hs[second : second + ROWS, :]
                )
            )
        rows.append(jnp.concatenate(tiles, axis=1))
    heads = jnp.concatenate(rows, axis=0).astype(jnp.bfloat16)
    wo_copy.wait()
    result = jnp.dot(heads, wo[...], preferred_element_type=jnp.float32)
    for j in range(DRAFT):
        out[j] = result[j * ROWS : (j + 1) * ROWS, :].astype(jnp.bfloat16)


def attend(lens, hidden, gain, cosine, sine, wq, wkv, wo, kv):
    hbm = pl.BlockSpec(memory_space=pltpu.HBM)
    vmem = pl.BlockSpec(memory_space=pltpu.VMEM)
    return pl.pallas_call(
        attend_kernel,
        out_shape=jax.ShapeDtypeStruct((DRAFT, ROWS, D), jnp.bfloat16),
        in_specs=[pl.BlockSpec(memory_space=pltpu.SMEM)] + [vmem] * 4 + [hbm] * 4,
        out_specs=vmem,
        scratch_shapes=[
            pltpu.VMEM((D, QH * HD), jnp.bfloat16),
            pltpu.VMEM((D, KH * 2 * HD), jnp.bfloat16),
            pltpu.VMEM((QH * HD, D), jnp.bfloat16),
            pltpu.VMEM((ROWS, SLOTS, 128), jnp.bfloat16),
            pltpu.VMEM((4 * QH * ROWS, 128), jnp.float32),
            pltpu.VMEM((DRAFT * KH * ROWS, 128), jnp.float32),
            pltpu.VMEM((4 * QH * ROWS, 128), jnp.float32),
            pltpu.VMEM((4 * QH, SLOTS), jnp.float32),
            pltpu.SemaphoreType.DMA((17,)),
        ],
        compiler_params=pltpu.CompilerParams(vmem_limit_bytes=VMEM_LIMIT),
        cost_estimate=pl.CostEstimate(flops=400_000_000, transcendentals=800_000, bytes_accessed=13_500_000),
        name="attend",
    )(lens, hidden, gain, cosine, sine, wq, wkv, wo, kv)


def mlp_kernel(tokens, gathered, out, weights, sems):
    copies = [
        pltpu.make_async_copy(gathered.at[h, z], weights.at[z, :, h], sems.at[2 * z + h])
        for z in range(Z)
        for h in range(2)
    ]
    for c in copies:
        c.start()
    count = tokens.shape[0]
    gate = jnp.zeros((count, FFS), jnp.float32)
    up = jnp.zeros((count, FFS), jnp.float32)
    for z in range(Z):
        copies[2 * z].wait()
        copies[2 * z + 1].wait()
        part = tokens[:, z * 256 : (z + 1) * 256]
        gate = gate + jnp.dot(
            part, weights[z, :, :, 0:16, :].reshape(256, FFS), preferred_element_type=jnp.float32
        )
        up = up + jnp.dot(
            part, weights[z, :, :, 16:32, :].reshape(256, FFS), preferred_element_type=jnp.float32
        )
    act = (gate / (1.0 + jnp.exp(-gate)) * up).astype(jnp.bfloat16)
    for z in range(Z):
        down = weights[z, :, :, 32:48, :].reshape(256, FFS)
        out[:, z * 256 : (z + 1) * 256] = lax.dot_general(
            act, down, (((1,), (1,)), ((), ())), preferred_element_type=jnp.float32
        ).astype(jnp.bfloat16)


def mlp(tokens, gathered):
    vmem = pl.BlockSpec(memory_space=pltpu.VMEM)
    return pl.pallas_call(
        mlp_kernel,
        out_shape=jax.ShapeDtypeStruct(tokens.shape, jnp.bfloat16),
        in_specs=[vmem, pl.BlockSpec(memory_space=pltpu.HBM)],
        out_specs=vmem,
        scratch_shapes=[
            pltpu.VMEM((Z, 8, 2, 48, FFS), jnp.bfloat16),
            pltpu.SemaphoreType.DMA((2 * Z,)),
        ],
        compiler_params=pltpu.CompilerParams(vmem_limit_bytes=VMEM_LIMIT),
        cost_estimate=pl.CostEstimate(flops=400_000_000, transcendentals=32768, bytes_accessed=4_200_000),
        name="mlp",
    )(tokens, gathered)


def after(first, then):
    return lax.optimization_barrier((first, then))[1]


def normalize(hidden, gain):
    wide = hidden.astype(jnp.float32)
    factor = lax.rsqrt(jnp.mean(wide * wide, axis=-1, keepdims=True) + EPS)
    return (wide * factor * gain).astype(jnp.bfloat16)


def local(
    exit_hidden,
    exit_depth,
    context_len,
    attn_gain,
    w_query,
    w_keyval,
    w_out,
    kv_cache,
    mlp_gain,
    w_gate,
    w_up,
    w_down,
):
    section = lax.axis_index("section")
    tensor = lax.axis_index("tensor")

    rows = jnp.stack([w_gate[0], w_up[0], w_down[0]])
    sliced = rows.reshape(3, 2, 16, 8, FFS).transpose(1, 3, 0, 2, 4).reshape(16, 48, FFS)
    blocks = lax.all_to_all(sliced, ("section", "y", "xh"), 0, 0, tiled=True)
    blocks = blocks.reshape(2, 8, 48, FFS)

    def gathered(block):
        return lax.all_gather(block, ("section", "z"), axis=0).reshape(2, Z, 8, 48, FFS)

    weights = [gathered(blocks[0])]

    mine = exit_hidden.transpose(1, 0, 2).reshape(TOKENS, 512)
    entry = lax.all_to_all(
        jnp.broadcast_to(mine[None], (4, TOKENS, 512)), CHIP, 0, 0, tiled=True
    )
    whole = entry.transpose(1, 0, 2).reshape(TOKENS, D)

    where_at = (jnp.arange(DRAFT, dtype=jnp.int32)[:, None] + context_len[None, :]).reshape(TOKENS)
    rates = jnp.exp(jnp.arange(HD // 2, dtype=jnp.float32) * (-2.0 * math.log(THETA) / HD))
    angles = where_at.astype(jnp.float32)[:, None] * rates
    c = jnp.cos(angles)
    s = jnp.sin(angles)
    cosine = jnp.concatenate([c, c, c, c], axis=1)
    sine = jnp.concatenate([-s, s, -s, s], axis=1)

    cache = kv_cache[0].reshape(ROWS, SLOTS, 128)
    other_gain = lax.ppermute(mlp_gain, "section", [(0, 1), (1, 0)])
    gains = [jnp.where(section == l, mlp_gain, other_gain) for l in range(2)]

    piece = section * 2 + tensor
    kept = lax.dynamic_slice_in_dim(whole, piece * ROWS, ROWS, 0)
    states = []
    for l in range(2):
        partial = attend(
            context_len, whole, attn_gain, cosine, sine, w_query[0], w_keyval[0], w_out[0], cache
        )
        parts = lax.all_to_all(partial, CHIP, 0, 0, tiled=True)
        mid = (
            kept.astype(jnp.float32)
            + parts[2 * l].astype(jnp.float32)
            + parts[2 * l + 1].astype(jnp.float32)
        ).astype(jnp.bfloat16)
        if l == 0:
            weights.append(gathered(after(mid, blocks[1])))
        mlp_in = normalize(mid, gains[l])
        everyone = lax.all_to_all(
            jnp.broadcast_to(mlp_in[None], (16, ROWS, D)), PLANE, 0, 0, tiled=True
        )
        share = mlp(everyone.reshape(16 * ROWS, D), weights[l])
        shares = lax.all_to_all(share.reshape(16, ROWS, D), PLANE, 0, 0, tiled=True)
        updated = (mid.astype(jnp.float32) + jnp.sum(shares.astype(jnp.float32), axis=0)).astype(
            jnp.bfloat16
        )
        kept = jnp.where((exit_depth <= l)[:, None], updated, kept)
        if l == 0:
            spread = lax.all_to_all(
                jnp.broadcast_to(kept[None], (4, ROWS, D)), CHIP, 0, 0, tiled=True
            )
            whole = spread.reshape(TOKENS, D)
            states.append(
                lax.dynamic_slice_in_dim(spread, tensor * (D // 2), D // 2, 2)
            )
        else:
            halves = kept.reshape(ROWS, 2, D // 2).transpose(1, 0, 2)
            spread = lax.all_to_all(
                jnp.concatenate([halves, halves]), CHIP, 0, 0, tiled=True
            )
            states.append(spread)
    result = jnp.where(section == 0, states[0], states[1])
    return result.transpose(1, 0, 2)[None]


def solution(mesh):
    wide = Mesh(mesh.devices.reshape(2, 2, Z, 4, 2), ("section", "tensor", "z", "y", "xh"))
    dp = ("z", "y", "xh")
    in_specs = (
        P(dp, None, ("section", "tensor")),
        P(dp),
        P(dp),
        P("section", None),
        P("section", None, "tensor"),
        P("section", None, "tensor"),
        P("section", "tensor", None),
        P("section", dp, None, "tensor", None),
        P("section", None),
        P("section", dp, "tensor"),
        P("section", dp, "tensor"),
        P("section", dp, "tensor"),
    )
    out_specs = P("section", dp, None, "tensor")
    return jax.shard_map(local, mesh=wide, in_specs=in_specs, out_specs=out_specs, check_vma=False)
```

```python
import functools
import math

import jax
import jax.numpy as jnp
from jax import lax
from jax.experimental import pallas as pl
from jax.experimental.pallas import tpu as pltpu
from jax.sharding import Mesh, PartitionSpec as P

D = 2048
DRAFT = 4
CTX = 384
ROWS = 8
TOKENS = ROWS * DRAFT
HD = 64
QH = 16
KH = 4
SLOTS = CTX * KH
VMEM_LIMIT = 60 * 1024 * 1024
AHEAD = 5
FFS = 256
EPS = 1e-05
THETA = 500000.0
NEGATIVE = -1e30
GROUPS = ((("tensor", "y", "xh"), 16), (("tensor", "y"), 8))
CHIP = ("section", "tensor")
Z = 8


def attend_kernel(
    by_token, lens, me, *refs
):
    pieces, refs = refs[:4], refs[4:]
    gain_h, cos_h, sin_h, wq_h, wkv_h, wo_h, kv_h, *refs = refs
    out, refs = refs[:4], refs[4:]
    kept, half, *refs = refs
    hidden, gain, cosine, sine, wq, wkv, wo, kv, qs, nk, hs, bias, result, sems = refs
    mine = me[0]
    small = []
    small.append(pltpu.make_async_copy(gain_h, gain, sems.at[4]))
    small.append(pltpu.make_async_copy(cos_h, cosine, sems.at[5]))
    small.append(pltpu.make_async_copy(sin_h, sine, sems.at[6]))
    chunks = 8
    step = D // chunks
    copies = []
    for p in range(chunks):
        at = pl.ds(p * step, step)
        copies.append(pltpu.make_async_copy(wq_h.at[at], wq.at[at], sems.at[7 + 2 * p]))
        copies.append(pltpu.make_async_copy(wkv_h.at[at], wkv.at[at], sems.at[8 + 2 * p]))
    base = 7 + 2 * chunks
    kv_copies = [
        pltpu.make_async_copy(kv_h.at[r], kv.at[r], sems.at[base + r]) for r in range(ROWS)
    ]
    wo_copies = [
        pltpu.make_async_copy(
            wo_h.at[pl.ds(p * 256, 256)], wo.at[pl.ds(p * 256, 256)], sems.at[base + ROWS + p]
        )
        for p in range(4)
    ]
    queue = [copies[2 * p : 2 * p + 2] for p in range(chunks)] + [
        kv_copies[2 * p : 2 * p + 2] for p in range(ROWS // 2)
    ]
    queue += [[c] for c in wo_copies]
    for c in small:
        c.start()
    for group in queue[:AHEAD]:
        for c in group:
            c.start()

    def arrived(n):
        for c in queue[n]:
            c.wait()
        if n + AHEAD < len(queue):
            for c in queue[n + AHEAD]:
                c.start()

    row = lax.broadcasted_iota(jnp.int32, (4 * QH, SLOTS), 0)
    place = lax.broadcasted_iota(jnp.int32, (4 * QH, SLOTS), 1)
    bias[...] = jnp.where((place & 3) == (row >> 4), 0.0, NEGATIVE)
    new_row = lax.broadcasted_iota(jnp.int32, (4 * QH, DRAFT * KH), 0)
    new_col = lax.broadcasted_iota(jnp.int32, (4 * QH, DRAFT * KH), 1)
    seen = ((new_col & 3) == (new_row >> 4)) & ((new_col >> 2) <= (new_row & 3))

    for k in range(4):
        other = mine ^ k
        if by_token:
            hidden[other] = pieces[k][...]
        else:
            hidden[:, :, pl.ds(pl.multiple_of(other * 512, 512), 512)] = pieces[k][...]
    for c in small:
        c.wait()
    kept[...] = hidden[mine]
    if by_token:
        half[...] = jnp.where((mine & 1) == 0, hidden[:, :, : D // 2], hidden[:, :, D // 2 :])
    wide = hidden[...].astype(jnp.float32).reshape(TOKENS, D)
    factor = lax.rsqrt(jnp.mean(wide * wide, axis=-1, keepdims=True) + EPS)
    normed = (wide * factor * gain[...]).astype(jnp.bfloat16)
    q = jnp.zeros((TOKENS, QH * HD), jnp.float32)
    new = jnp.zeros((TOKENS, KH * 2 * HD), jnp.float32)
    for p in range(chunks):
        at = pl.ds(p * step, step)
        arrived(p)
        part = normed[:, p * step : (p + 1) * step]
        q = q + jnp.dot(part, wq[at], preferred_element_type=jnp.float32)
        new = new + jnp.dot(part, wkv[at], preferred_element_type=jnp.float32)

    lane = lax.broadcasted_iota(jnp.int32, (TOKENS, 128), 1)
    low = (lane & 63) < 32
    left = lane < HD
    cos_all = cosine[...]
    sin_all = sine[...]

    def turned(block, c, s):
        other = jnp.where(low, pltpu.roll(block, 96, 1), pltpu.roll(block, 32, 1))
        return block * c + other * s

    scale = HD ** (-0.5)
    for m in range(QH // 2):
        block = turned(q[:, m * 128 : (m + 1) * 128], cos_all, sin_all) * scale
        pair = (jnp.where(left, block, 0.0), jnp.where(left, pltpu.roll(block, HD, 1), 0.0))
        for half in range(2):
            for j in range(DRAFT):
                at = ((2 * m + half) * DRAFT + j) * ROWS
                qs[at : at + ROWS, :] = pair[half][j * ROWS : (j + 1) * ROWS, :]
    key_cos = jnp.where(left, cos_all, 1.0)
    key_sin = jnp.where(left, sin_all, 0.0)
    for h in range(KH):
        block = turned(new[:, h * 128 : (h + 1) * 128], key_cos, key_sin)
        for i in range(DRAFT):
            at = (i * KH + h) * ROWS
            nk[at : at + ROWS, :] = block[i * ROWS : (i + 1) * ROWS, :]

    last = (((1,), (1,)), ((), ()))
    for r in range(ROWS):
        fresh = nk[pl.ds(r, DRAFT * KH, stride=ROWS), :].astype(jnp.bfloat16)
        asked = qs[pl.ds(r, 4 * QH, stride=ROWS), :].astype(jnp.bfloat16)
        if r % 2 == 0:
            arrived(chunks + r // 2)
        stored = kv[r]
        scores = lax.dot_general(asked, stored, last, preferred_element_type=jnp.float32)
        scores = jnp.where(place < KH * lens[r], scores, NEGATIVE) + bias[...]
        new_scores = lax.dot_general(asked, fresh, last, preferred_element_type=jnp.float32)
        new_scores = jnp.where(seen, new_scores, NEGATIVE)
        top = jnp.maximum(
            jnp.max(scores, axis=-1, keepdims=True), jnp.max(new_scores, axis=-1, keepdims=True)
        )
        weights = jnp.exp(scores - top)
        new_weights = jnp.exp(new_scores - top)
        total = jnp.sum(weights, axis=-1, keepdims=True) + jnp.sum(
            new_weights, axis=-1, keepdims=True
        )
        mixed = jnp.dot(
            weights.astype(jnp.bfloat16), stored, preferred_element_type=jnp.float32
        ) + jnp.dot(new_weights.astype(jnp.bfloat16), fresh, preferred_element_type=jnp.float32)
        hs[pl.ds(r, 4 * QH, stride=ROWS), :] = mixed / total

    side = lax.broadcasted_iota(jnp.int32, (ROWS, 128), 1) < HD
    rows = []
    for j in range(DRAFT):
        tiles = []
        for m in range(QH // 2):
            first = ((2 * m) * DRAFT + j) * ROWS
            second = ((2 * m + 1) * DRAFT + j) * ROWS
            tiles.append(
                jnp.where(
                    side, pltpu.roll(hs[first : first + ROWS, :], HD, 1), hs[second : second + ROWS, :]
                )
            )
        rows.append(jnp.concatenate(tiles, axis=1))
    heads = jnp.concatenate(rows, axis=0).astype(jnp.bfloat16)
    for p in range(4):
        arrived(chunks + ROWS // 2 + p)
    shares = jnp.dot(heads, wo[...], preferred_element_type=jnp.float32)
    for j in range(DRAFT):
        result[j] = shares[j * ROWS : (j + 1) * ROWS, :].astype(jnp.bfloat16)
    for k in range(4):
        out[k][...] = result[mine ^ k]


def attend(by_token, lens, me, pieces, gain, cosine, sine, wq, wkv, wo, kv):
    hbm = pl.BlockSpec(memory_space=pltpu.HBM)
    vmem = pl.BlockSpec(memory_space=pltpu.VMEM)
    smem = pl.BlockSpec(memory_space=pltpu.SMEM)
    quarter = jax.ShapeDtypeStruct((ROWS, D), jnp.bfloat16)
    return pl.pallas_call(
        functools.partial(attend_kernel, by_token),
        out_shape=[quarter] * 5 + [jax.ShapeDtypeStruct((DRAFT, ROWS, D // 2), jnp.bfloat16)],
        in_specs=[smem] * 2 + [vmem] * 4 + [hbm] * 7,
        out_specs=[vmem] * 6,
        scratch_shapes=[
            pltpu.VMEM((DRAFT, ROWS, D), jnp.bfloat16),
            pltpu.VMEM((1, D), jnp.float32),
            pltpu.VMEM((TOKENS, 128), jnp.float32),
            pltpu.VMEM((TOKENS, 128), jnp.float32),
            pltpu.VMEM((D, QH * HD), jnp.bfloat16),
            pltpu.VMEM((D, KH * 2 * HD), jnp.bfloat16),
            pltpu.VMEM((QH * HD, D), jnp.bfloat16),
            pltpu.VMEM((ROWS, SLOTS, 128), jnp.bfloat16),
            pltpu.VMEM((4 * QH * ROWS, 128), jnp.float32),
            pltpu.VMEM((DRAFT * KH * ROWS, 128), jnp.float32),
            pltpu.VMEM((4 * QH * ROWS, 128), jnp.float32),
            pltpu.VMEM((4 * QH, SLOTS), jnp.float32),
            pltpu.VMEM((DRAFT, ROWS, D), jnp.bfloat16),
            pltpu.SemaphoreType.DMA((35,)),
        ],
        compiler_params=pltpu.CompilerParams(vmem_limit_bytes=VMEM_LIMIT),
        cost_estimate=pl.CostEstimate(flops=400_000_000, transcendentals=800_000, bytes_accessed=13_500_000),
        name="attend",
    )(lens, me, *pieces, gain, cosine, sine, wq, wkv, wo, kv)


def mlp_kernel(tokens_h, gathered, out, tokens, weights, sems):
    token_copy = pltpu.make_async_copy(tokens_h, tokens, sems.at[2 * Z])
    token_copy.start()
    copies = [
        pltpu.make_async_copy(gathered.at[h, z], weights.at[z, :, h], sems.at[2 * z + h])
        for z in range(Z)
        for h in range(2)
    ]
    for c in copies:
        c.start()
    token_copy.wait()
    count = tokens.shape[0]
    units = weights.shape[-1]
    gate = jnp.zeros((count, units), jnp.float32)
    up = jnp.zeros((count, units), jnp.float32)
    for z in range(Z):
        copies[2 * z].wait()
        copies[2 * z + 1].wait()
        part = tokens[:, z * 256 : (z + 1) * 256]
        gate = gate + jnp.dot(
            part, weights[z, :, :, 0:16, :].reshape(256, units), preferred_element_type=jnp.float32
        )
        up = up + jnp.dot(
            part, weights[z, :, :, 16:32, :].reshape(256, units), preferred_element_type=jnp.float32
        )
    act = (gate / (1.0 + jnp.exp(-gate)) * up).astype(jnp.bfloat16)
    for z in range(Z):
        down = weights[z, :, :, 32:48, :].reshape(256, units)
        out[:, z * 256 : (z + 1) * 256] = lax.dot_general(
            act, down, (((1,), (1,)), ((), ())), preferred_element_type=jnp.float32
        ).astype(jnp.bfloat16)


def mlp(tokens, gathered):
    hbm = pl.BlockSpec(memory_space=pltpu.HBM)
    units = gathered.shape[-1]
    return pl.pallas_call(
        mlp_kernel,
        out_shape=jax.ShapeDtypeStruct(tokens.shape, jnp.bfloat16),
        in_specs=[hbm, hbm],
        out_specs=pl.BlockSpec(memory_space=pltpu.VMEM),
        scratch_shapes=[
            pltpu.VMEM(tokens.shape, jnp.bfloat16),
            pltpu.VMEM((Z, 8, 2, 48, units), jnp.bfloat16),
            pltpu.SemaphoreType.DMA((2 * Z + 1,)),
        ],
        compiler_params=pltpu.CompilerParams(vmem_limit_bytes=VMEM_LIMIT),
        cost_estimate=pl.CostEstimate(flops=400_000_000, transcendentals=32768, bytes_accessed=4_200_000),
        name="mlp",
    )(tokens, gathered)


def after(first, then):
    return lax.optimization_barrier((first, then))[1]


def exchanged(blocks):
    return [
        lax.ppermute(blocks[k], CHIP, [(i, i ^ k) for i in range(4)]) for k in (1, 2, 3)
    ]


def normalize(hidden, gain):
    wide = hidden.astype(jnp.float32)
    factor = lax.rsqrt(jnp.mean(wide * wide, axis=-1, keepdims=True) + EPS)
    return (wide * factor * gain).astype(jnp.bfloat16)


def local(
    exit_hidden,
    exit_depth,
    context_len,
    attn_gain,
    w_query,
    w_keyval,
    w_out,
    kv_cache,
    mlp_gain,
    w_gate,
    w_up,
    w_down,
):
    section = lax.axis_index("section")
    tensor = lax.axis_index("tensor")

    def half_rows(which):
        return jnp.stack(
            [lax.dynamic_slice_in_dim(w[0], which * 16, 16, 0) for w in (w_gate, w_up, w_down)]
        )

    own_half = half_rows(section)
    got_half = lax.ppermute(half_rows(1 - section), "section", [(0, 1), (1, 0)])
    first = jnp.where(section == 0, own_half, got_half)
    second = jnp.where(section == 1, own_half, got_half)
    block0 = lax.all_to_all(
        first.reshape(3, 16, 8, FFS).transpose(2, 0, 1, 3).reshape(8, 48, FFS),
        ("y", "xh"),
        0,
        0,
        tiled=True,
    )

    def gathered(block):
        g = lax.all_gather(block, ("section", "z"), axis=0)
        return g.reshape(2, Z, 8, 48, block.shape[-1])

    weights = [gathered(block0)]

    other_gain = lax.ppermute(mlp_gain, "section", [(0, 1), (1, 0)])
    gains = [jnp.where(section == l, mlp_gain, other_gain) for l in range(2)]
    own_piece = after(block0, exit_hidden.transpose(1, 0, 2))
    pieces = [own_piece] + exchanged([own_piece] * 4)
    slices = second.reshape(3, 16, 4, 2 * FFS).transpose(2, 0, 1, 3).reshape(4, 1, 48, 2 * FFS)
    slices = jnp.broadcast_to(slices, (4, 2, 48, 2 * FFS)).reshape(8, 48, 2 * FFS)
    block1 = lax.all_to_all(after(pieces[3], slices), ("y", "xh"), 0, 0, tiled=True)

    where_at = (jnp.arange(DRAFT, dtype=jnp.int32)[:, None] + context_len[None, :]).reshape(TOKENS)
    rates = jnp.exp(jnp.arange(HD // 2, dtype=jnp.float32) * (-2.0 * math.log(THETA) / HD))
    angles = where_at.astype(jnp.float32)[:, None] * rates
    c = jnp.cos(angles)
    s = jnp.sin(angles)
    cosine = jnp.concatenate([c, c, c, c], axis=1)
    sine = jnp.concatenate([-s, s, -s, s], axis=1)

    cache = kv_cache[0].reshape(ROWS, SLOTS, 128)
    me = section * 2 + tensor
    for l in range(2):
        *partial, before, half = attend(
            l == 1,
            context_len,
            me.reshape(1),
            pieces,
            attn_gain,
            cosine,
            sine,
            w_query[0],
            w_keyval[0],
            w_out[0],
            cache,
        )
        near, across, far = exchanged(partial)
        mine = section == l
        mid = (
            before.astype(jnp.float32)
            + jnp.where(mine, partial[0], across).astype(jnp.float32)
            + jnp.where(mine, near, far).astype(jnp.float32)
        ).astype(jnp.bfloat16)
        if l == 0:
            weights.append(gathered(after(mid, block1)))
        mlp_in = normalize(mid, gains[l])
        axes, group = GROUPS[l]
        everyone = lax.all_to_all(
            jnp.broadcast_to(mlp_in[None], (group, ROWS, D)), axes, 0, 0, tiled=True
        )
        share = mlp(everyone.reshape(group * ROWS, D), weights[l])
        shares = lax.all_to_all(share.reshape(group, ROWS, D), axes, 0, 0, tiled=True)
        updated = (mid.astype(jnp.float32) + jnp.sum(shares.astype(jnp.float32), axis=0)).astype(
            jnp.bfloat16
        )
        kept = jnp.where((exit_depth <= l)[:, None], updated, before)
        if l == 0:
            pieces = [kept] + exchanged([kept] * 4)
    left, right = kept[:, : D // 2], kept[:, D // 2 :]
    same = jnp.where(tensor == 0, left, right)
    opposite = jnp.where(tensor == 0, right, left)
    near, across, far = exchanged([same, opposite, same, opposite])
    last = jnp.where(
        tensor == 0, jnp.stack([across, far, same, near]), jnp.stack([far, across, near, same])
    )
    return jnp.where(section == 0, half, last).transpose(1, 0, 2)[None]


def solution(mesh):
    wide = Mesh(mesh.devices.reshape(2, 2, Z, 4, 2), ("section", "tensor", "z", "y", "xh"))
    dp = ("z", "y", "xh")
    in_specs = (
        P(dp, None, ("section", "tensor")),
        P(dp),
        P(dp),
        P("section", None),
        P("section", None, "tensor"),
        P("section", None, "tensor"),
        P("section", "tensor", None),
        P("section", dp, None, "tensor", None),
        P("section", None),
        P("section", dp, "tensor"),
        P("section", dp, "tensor"),
        P("section", dp, "tensor"),
    )
    out_specs = P("section", dp, None, "tensor")
    return jax.shard_map(local, mesh=wide, in_specs=in_specs, out_specs=out_specs, check_vma=False)
```

```python
import functools
import math

import jax
import jax.numpy as jnp
from jax import lax
from jax.experimental import pallas as pl
from jax.experimental.pallas import tpu as pltpu
from jax.sharding import Mesh, PartitionSpec as P


D = 2048
DRAFT = 4
CTX = 384
ROWS = 8
TOKENS = ROWS * DRAFT
HD = 64
QH = 16
KH = 4
SLOTS = CTX * KH
VMEM_LIMIT = 53000 * 1024
AHEAD = 5
FFS = 256
EPS = 1e-05
THETA = 500000.0
NEGATIVE = -1e30
GROUPS = ((("tensor", "y", "xh"), 16), (("tensor", "y"), 8))
CHIP = ("section", "tensor")
Z = 8


def attend_kernel(
    by_token, lens, me, *refs
):
    pieces, refs = refs[:4], refs[4:]
    gain_h, cos_h, sin_h, wq_h, wkv_h, wo_h, kv_h, *refs = refs
    out, refs = refs[:4], refs[4:]
    kept, half, *refs = refs
    hidden, gain, cosine, sine, wq, wkv, wo, kv, qs, nk, hs, bias, result, sems = refs
    mine = me[0]
    small = []
    small.append(pltpu.make_async_copy(gain_h, gain, sems.at[4]))
    small.append(pltpu.make_async_copy(cos_h, cosine, sems.at[5]))
    small.append(pltpu.make_async_copy(sin_h, sine, sems.at[6]))
    chunks = 8
    step = D // chunks
    copies = []
    for p in range(chunks):
        at = pl.ds(p * step, step)
        copies.append(pltpu.make_async_copy(wq_h.at[at], wq.at[at], sems.at[7 + 2 * p]))
        copies.append(pltpu.make_async_copy(wkv_h.at[at], wkv.at[at], sems.at[8 + 2 * p]))
    base = 7 + 2 * chunks
    kv_copies = [
        pltpu.make_async_copy(kv_h.at[r], kv.at[r], sems.at[base + r]) for r in range(ROWS)
    ]
    wo_copies = [
        pltpu.make_async_copy(
            wo_h.at[pl.ds(p * 256, 256)], wo.at[pl.ds(p * 256, 256)], sems.at[base + ROWS + p]
        )
        for p in range(4)
    ]
    queue = [copies[2 * p : 2 * p + 2] for p in range(chunks)] + [
        kv_copies[2 * p : 2 * p + 2] for p in range(ROWS // 2)
    ]
    queue += [[c] for c in wo_copies]
    for c in small:
        c.start()
    for group in queue[:AHEAD]:
        for c in group:
            c.start()

    def arrived(n):
        for c in queue[n]:
            c.wait()
        if n + AHEAD < len(queue):
            for c in queue[n + AHEAD]:
                c.start()

    row = lax.broadcasted_iota(jnp.int32, (4 * QH, SLOTS), 0)
    place = lax.broadcasted_iota(jnp.int32, (4 * QH, SLOTS), 1)
    bias[...] = jnp.where((place & 3) == (row >> 4), 0.0, NEGATIVE)
    new_row = lax.broadcasted_iota(jnp.int32, (4 * QH, DRAFT * KH), 0)
    new_col = lax.broadcasted_iota(jnp.int32, (4 * QH, DRAFT * KH), 1)
    seen = ((new_col & 3) == (new_row >> 4)) & ((new_col >> 2) <= (new_row & 3))

    for k in range(4):
        other = mine ^ k
        if by_token:
            hidden[other] = pieces[k][...]
        else:
            hidden[:, :, pl.ds(pl.multiple_of(other * 512, 512), 512)] = pieces[k][...]
    for c in small:
        c.wait()
    kept[...] = hidden[mine]
    if by_token:
        half[...] = jnp.where((mine & 1) == 0, hidden[:, :, : D // 2], hidden[:, :, D // 2 :])
    wide = hidden[...].astype(jnp.float32).reshape(TOKENS, D)
    factor = lax.rsqrt(jnp.mean(wide * wide, axis=-1, keepdims=True) + EPS)
    normed = (wide * factor * gain[...]).astype(jnp.bfloat16)
    q = jnp.zeros((TOKENS, QH * HD), jnp.float32)
    new = jnp.zeros((TOKENS, KH * 2 * HD), jnp.float32)
    for p in range(chunks):
        at = pl.ds(p * step, step)
        arrived(p)
        part = normed[:, p * step : (p + 1) * step]
        q = q + jnp.dot(part, wq[at], preferred_element_type=jnp.float32)
        new = new + jnp.dot(part, wkv[at], preferred_element_type=jnp.float32)

    lane = lax.broadcasted_iota(jnp.int32, (TOKENS, 128), 1)
    low = (lane & 63) < 32
    left = lane < HD
    cos_all = cosine[...]
    sin_all = sine[...]

    def turned(block, c, s):
        other = jnp.where(low, pltpu.roll(block, 96, 1), pltpu.roll(block, 32, 1))
        return block * c + other * s

    scale = HD ** (-0.5)
    for m in range(QH // 2):
        block = turned(q[:, m * 128 : (m + 1) * 128], cos_all, sin_all) * scale
        pair = (jnp.where(left, block, 0.0), jnp.where(left, pltpu.roll(block, HD, 1), 0.0))
        for half in range(2):
            for j in range(DRAFT):
                at = ((2 * m + half) * DRAFT + j) * ROWS
                qs[at : at + ROWS, :] = pair[half][j * ROWS : (j + 1) * ROWS, :]
    key_cos = jnp.where(left, cos_all, 1.0)
    key_sin = jnp.where(left, sin_all, 0.0)
    for h in range(KH):
        block = turned(new[:, h * 128 : (h + 1) * 128], key_cos, key_sin)
        for i in range(DRAFT):
            at = (i * KH + h) * ROWS
            nk[at : at + ROWS, :] = block[i * ROWS : (i + 1) * ROWS, :]

    last = (((1,), (1,)), ((), ()))
    for r in range(ROWS):
        fresh = nk[pl.ds(r, DRAFT * KH, stride=ROWS), :].astype(jnp.bfloat16)
        asked = qs[pl.ds(r, 4 * QH, stride=ROWS), :].astype(jnp.bfloat16)
        if r % 2 == 0:
            arrived(chunks + r // 2)
        stored = kv[r]
        scores = lax.dot_general(asked, stored, last, preferred_element_type=jnp.float32)
        scores = jnp.where(place < KH * lens[r], scores, NEGATIVE) + bias[...]
        new_scores = lax.dot_general(asked, fresh, last, preferred_element_type=jnp.float32)
        new_scores = jnp.where(seen, new_scores, NEGATIVE)
        top = jnp.maximum(
            jnp.max(scores, axis=-1, keepdims=True), jnp.max(new_scores, axis=-1, keepdims=True)
        )
        weights = jnp.exp(scores - top)
        new_weights = jnp.exp(new_scores - top)
        total = jnp.sum(weights, axis=-1, keepdims=True) + jnp.sum(
            new_weights, axis=-1, keepdims=True
        )
        mixed = jnp.dot(
            weights.astype(jnp.bfloat16), stored, preferred_element_type=jnp.float32
        ) + jnp.dot(new_weights.astype(jnp.bfloat16), fresh, preferred_element_type=jnp.float32)
        hs[pl.ds(r, 4 * QH, stride=ROWS), :] = mixed / total

    side = lax.broadcasted_iota(jnp.int32, (ROWS, 128), 1) < HD
    rows = []
    for j in range(DRAFT):
        tiles = []
        for m in range(QH // 2):
            first = ((2 * m) * DRAFT + j) * ROWS
            second = ((2 * m + 1) * DRAFT + j) * ROWS
            tiles.append(
                jnp.where(
                    side, pltpu.roll(hs[first : first + ROWS, :], HD, 1), hs[second : second + ROWS, :]
                )
            )
        rows.append(jnp.concatenate(tiles, axis=1))
    heads = jnp.concatenate(rows, axis=0).astype(jnp.bfloat16)
    for p in range(4):
        arrived(chunks + ROWS // 2 + p)
    shares = jnp.dot(heads, wo[...], preferred_element_type=jnp.float32)
    for j in range(DRAFT):
        result[j] = shares[j * ROWS : (j + 1) * ROWS, :].astype(jnp.bfloat16)
    for k in range(4):
        out[k][...] = result[mine ^ k]


def attend(by_token, lens, me, pieces, gain, cosine, sine, wq, wkv, wo, kv):
    hbm = pl.BlockSpec(memory_space=pltpu.HBM)
    vmem = pl.BlockSpec(memory_space=pltpu.VMEM)
    smem = pl.BlockSpec(memory_space=pltpu.SMEM)
    quarter = jax.ShapeDtypeStruct((ROWS, D), jnp.bfloat16)
    return pl.pallas_call(
        functools.partial(attend_kernel, by_token),
        out_shape=[quarter] * 5 + [jax.ShapeDtypeStruct((DRAFT, ROWS, D // 2), jnp.bfloat16)],
        in_specs=[smem] * 2 + [vmem] * 4 + [hbm] * 7,
        out_specs=[vmem] * 6,
        scratch_shapes=[
            pltpu.VMEM((DRAFT, ROWS, D), jnp.bfloat16),
            pltpu.VMEM((1, D), jnp.float32),
            pltpu.VMEM((TOKENS, 128), jnp.float32),
            pltpu.VMEM((TOKENS, 128), jnp.float32),
            pltpu.VMEM((D, QH * HD), jnp.bfloat16),
            pltpu.VMEM((D, KH * 2 * HD), jnp.bfloat16),
            pltpu.VMEM((QH * HD, D), jnp.bfloat16),
            pltpu.VMEM((ROWS, SLOTS, 128), jnp.bfloat16),
            pltpu.VMEM((4 * QH * ROWS, 128), jnp.float32),
            pltpu.VMEM((DRAFT * KH * ROWS, 128), jnp.float32),
            pltpu.VMEM((4 * QH * ROWS, 128), jnp.float32),
            pltpu.VMEM((4 * QH, SLOTS), jnp.float32),
            pltpu.VMEM((DRAFT, ROWS, D), jnp.bfloat16),
            pltpu.SemaphoreType.DMA((35,)),
        ],
        compiler_params=pltpu.CompilerParams(vmem_limit_bytes=VMEM_LIMIT),
        cost_estimate=pl.CostEstimate(flops=400_000_000, transcendentals=800_000, bytes_accessed=13_500_000),
        name="attend",
    )(lens, me, *pieces, gain, cosine, sine, wq, wkv, wo, kv)


def mlp_kernel(halves, tokens, gathered, out, weights, sems):
    copies = [
        pltpu.make_async_copy(gathered.at[h, z], weights.at[z, :, h], sems.at[2 * z + h])
        for z in range(Z)
        for h in range(2)
    ]
    for c in copies:
        c.start()
    count = tokens.shape[0]
    units = weights.shape[-1]
    gate = jnp.zeros((count, units), jnp.float32)
    up = jnp.zeros((count, units), jnp.float32)
    for z in range(Z):
        copies[2 * z].wait()
        copies[2 * z + 1].wait()
        part = tokens[:, z * 256 : (z + 1) * 256]
        gate = gate + jnp.dot(
            part, weights[z, :, :, 0:16, :].reshape(256, units), preferred_element_type=jnp.float32
        )
        up = up + jnp.dot(
            part, weights[z, :, :, 16:32, :].reshape(256, units), preferred_element_type=jnp.float32
        )
    act = (gate / (1.0 + jnp.exp(-gate)) * up).astype(jnp.bfloat16)
    for z in range(Z):
        down = weights[z, :, :, 32:48, :].reshape(256, units)
        share = lax.dot_general(
            act, down, (((1,), (1,)), ((), ())), preferred_element_type=jnp.float32
        ).astype(jnp.bfloat16)
        if halves:
            share = share.reshape(2, count // (2 * ROWS), ROWS, 256)
            at = (z % 4) * 256
            for side in range(2):
                out[z // 4, :, side, :, at : at + 256] = share[side]
        else:
            out[:, z * 256 : (z + 1) * 256] = share


def mlp(tokens, gathered, halves):
    hbm = pl.BlockSpec(memory_space=pltpu.HBM)
    vmem = pl.BlockSpec(memory_space=pltpu.VMEM)
    units = gathered.shape[-1]
    return pl.pallas_call(
        functools.partial(mlp_kernel, halves),
        out_shape=jax.ShapeDtypeStruct(
            (2, tokens.shape[0] // (2 * ROWS), 2, ROWS, D // 2) if halves else tokens.shape,
            jnp.bfloat16,
        ),
        in_specs=[vmem, hbm],
        out_specs=vmem,
        scratch_shapes=[
            pltpu.VMEM((Z, 8, 2, 48, units), jnp.bfloat16),
            pltpu.SemaphoreType.DMA((2 * Z,)),
        ],
        compiler_params=pltpu.CompilerParams(vmem_limit_bytes=VMEM_LIMIT),
        cost_estimate=pl.CostEstimate(flops=400_000_000, transcendentals=32768, bytes_accessed=4_200_000),
        name="mlp",
    )(tokens, gathered)


def after(first, then):
    return lax.optimization_barrier((first, then))[1]


def exchanged(blocks):
    return [
        lax.ppermute(blocks[k], CHIP, [(i, i ^ k) for i in range(4)]) for k in (1, 2, 3)
    ]


def normalize(hidden, gain):
    wide = hidden.astype(jnp.float32)
    factor = lax.rsqrt(jnp.mean(wide * wide, axis=-1, keepdims=True) + EPS)
    return (wide * factor * gain).astype(jnp.bfloat16)


def local(
    exit_hidden,
    exit_depth,
    context_len,
    attn_gain,
    w_query,
    w_keyval,
    w_out,
    kv_cache,
    mlp_gain,
    w_gate,
    w_up,
    w_down,
):
    section = lax.axis_index("section")
    tensor = lax.axis_index("tensor")

    def half_rows(which):
        return jnp.stack(
            [lax.dynamic_slice_in_dim(w[0], which * 16, 16, 0) for w in (w_gate, w_up, w_down)]
        )

    own_half = half_rows(section)
    got_half = lax.ppermute(half_rows(1 - section), "section", [(0, 1), (1, 0)])
    first = jnp.where(section == 0, own_half, got_half)
    second = jnp.where(section == 1, own_half, got_half)
    block0 = lax.all_to_all(
        first.reshape(3, 16, 8, FFS).transpose(2, 0, 1, 3).reshape(8, 48, FFS),
        ("y", "xh"),
        0,
        0,
        tiled=True,
    )

    other_gain = lax.ppermute(mlp_gain, "section", [(0, 1), (1, 0)])
    gains = [jnp.where(section == l, mlp_gain, other_gain) for l in range(2)]
    own_piece = exit_hidden.transpose(1, 0, 2)
    pieces = [own_piece] + exchanged([own_piece] * 4)

    def gathered(block):
        g = lax.all_gather(block, ("section", "z"), axis=0)
        return g.reshape(2, Z, 8, 48, block.shape[-1])

    weights = [gathered(after((pieces, other_gain), block0))]
    slices = second.reshape(3, 16, 4, 2 * FFS).transpose(2, 0, 1, 3).reshape(4, 1, 48, 2 * FFS)
    slices = jnp.broadcast_to(slices, (4, 2, 48, 2 * FFS)).reshape(8, 48, 2 * FFS)
    block1 = lax.all_to_all(after(pieces[3], slices), ("y", "xh"), 0, 0, tiled=True)

    where_at = (jnp.arange(DRAFT, dtype=jnp.int32)[:, None] + context_len[None, :]).reshape(TOKENS)
    rates = jnp.exp(jnp.arange(HD // 2, dtype=jnp.float32) * (-2.0 * math.log(THETA) / HD))
    angles = where_at.astype(jnp.float32)[:, None] * rates
    c = jnp.cos(angles)
    s = jnp.sin(angles)
    cosine = jnp.concatenate([c, c, c, c], axis=1)
    sine = jnp.concatenate([-s, s, -s, s], axis=1)

    cache = kv_cache[0].reshape(ROWS, SLOTS, 128)
    me = section * 2 + tensor
    for l in range(2):
        *partial, before, half = attend(
            l == 1,
            context_len,
            me.reshape(1),
            pieces,
            attn_gain,
            cosine,
            sine,
            w_query[0],
            w_keyval[0],
            w_out[0],
            cache,
        )
        near, across, far = exchanged(partial)
        mine = section == l
        mid = (
            before.astype(jnp.float32)
            + jnp.where(mine, partial[0], across).astype(jnp.float32)
            + jnp.where(mine, near, far).astype(jnp.float32)
        ).astype(jnp.bfloat16)
        if l == 0:
            weights.append(gathered(after(mid, block1)))
        mlp_in = normalize(mid, gains[l])
        axes, group = GROUPS[l]
        everyone = lax.all_to_all(
            jnp.broadcast_to(mlp_in[None], (group, ROWS, D)), axes, 0, 0, tiled=True
        )
        share = mlp(everyone.reshape(group * ROWS, D), weights[l], l == 1)
        if l == 0:
            shares = lax.all_to_all(share.reshape(group, ROWS, D), axes, 0, 0, tiled=True)
            total = jnp.sum(shares.astype(jnp.float32), axis=0)
            updated = (mid.astype(jnp.float32) + total).astype(jnp.bfloat16)
            kept = jnp.where((exit_depth <= l)[:, None], updated, before)
            pieces = [kept] + exchanged([kept] * 4)
    left, right = mid[:, : D // 2], mid[:, D // 2 :]
    same = jnp.where(tensor == 0, left, right)
    opposite = jnp.where(tensor == 0, right, left)
    got = lax.ppermute(opposite, "tensor", [(0, 1), (1, 0)])
    mids = jnp.where(tensor == 0, jnp.stack([same, got]), jnp.stack([got, same]))
    shares = lax.all_to_all(share.reshape(8, 2, ROWS, D // 2), axes, 0, 0, tiled=True)
    total = jnp.sum(shares.astype(jnp.float32), axis=0)
    updated = (mids.astype(jnp.float32) + total).astype(jnp.bfloat16)
    sent = lax.ppermute(updated, "section", [(0, 1)])
    last = jnp.concatenate([sent, updated])
    return jnp.where(section == 0, half, last).transpose(1, 0, 2)[None]


def solution(mesh):
    wide = Mesh(mesh.devices.reshape(2, 2, Z, 4, 2), ("section", "tensor", "z", "y", "xh"))
    dp = ("z", "y", "xh")
    in_specs = (
        P(dp, None, ("section", "tensor")),
        P(dp),
        P(dp),
        P("section", None),
        P("section", None, "tensor"),
        P("section", None, "tensor"),
        P("section", "tensor", None),
        P("section", dp, None, "tensor", None),
        P("section", None),
        P("section", dp, "tensor"),
        P("section", dp, "tensor"),
        P("section", dp, "tensor"),
    )
    out_specs = P("section", dp, None, "tensor")

    return jax.shard_map(local, mesh=wide, in_specs=in_specs, out_specs=out_specs, check_vma=False)
```

```python
import functools
import math

import jax
import jax.numpy as jnp
from jax import lax
from jax.experimental import pallas as pl
from jax.experimental.pallas import tpu as pltpu
from jax.sharding import Mesh, PartitionSpec as P


D = 2048
DRAFT = 4
CTX = 384
ROWS = 8
TOKENS = ROWS * DRAFT
HD = 64
QH = 16
KH = 4
SLOTS = CTX * KH
VMEM_LIMIT = 53000 * 1024
AHEAD = 8
FFS = 256
EPS = 1e-05
THETA = 500000.0
NEGATIVE = -1e30
GROUPS = ((("tensor", "y", "xh"), 16), (("tensor", "y"), 8))
CHIP = ("section", "tensor")
Z = 8


def attend_kernel(
    by_token, lens, me, *refs
):
    pieces, refs = refs[:4], refs[4:]
    gain_h, cos_h, sin_h, wq_h, wkv_h, wo_h, kv_h, *refs = refs
    out, refs = refs[:4], refs[4:]
    kept, half, *refs = refs
    hidden, gain, cosine, sine, wq, wkv, wo, kv, qs, nk, hs, slot, result, sems = refs
    mine = me[0]
    small = []
    small.append(pltpu.make_async_copy(gain_h, gain, sems.at[4]))
    small.append(pltpu.make_async_copy(cos_h, cosine, sems.at[5]))
    small.append(pltpu.make_async_copy(sin_h, sine, sems.at[6]))
    chunks = 8
    step = D // chunks
    copies = []
    for p in range(chunks):
        at = pl.ds(p * step, step)
        copies.append(pltpu.make_async_copy(wq_h.at[at], wq.at[at], sems.at[7 + 2 * p]))
        copies.append(pltpu.make_async_copy(wkv_h.at[at], wkv.at[at], sems.at[8 + 2 * p]))
    base = 7 + 2 * chunks
    kv_copies = [
        pltpu.make_async_copy(kv_h.at[r], kv.at[r], sems.at[base + r]) for r in range(ROWS)
    ]
    wo_copies = [
        pltpu.make_async_copy(
            wo_h.at[pl.ds(p * 256, 256)], wo.at[pl.ds(p * 256, 256)], sems.at[base + ROWS + p]
        )
        for p in range(4)
    ]
    queue = [copies[2 * p : 2 * p + 2] for p in range(chunks)] + [
        kv_copies[2 * p : 2 * p + 2] for p in range(ROWS // 2)
    ]
    queue += [[c] for c in wo_copies]
    for c in small:
        c.start()
    for group in queue[:AHEAD]:
        for c in group:
            c.start()

    def arrived(n):
        for c in queue[n]:
            c.wait()
        if n + AHEAD < len(queue):
            for c in queue[n + AHEAD]:
                c.start()

    row = lax.broadcasted_iota(jnp.int32, (4 * QH, SLOTS), 0)
    place = lax.broadcasted_iota(jnp.int32, (4 * QH, SLOTS), 1)
    slot[...] = jnp.where((place & 3) == (row >> 4), place, SLOTS)
    new_row = lax.broadcasted_iota(jnp.int32, (4 * QH, DRAFT * KH), 0)
    new_col = lax.broadcasted_iota(jnp.int32, (4 * QH, DRAFT * KH), 1)
    seen = ((new_col & 3) == (new_row >> 4)) & ((new_col >> 2) <= (new_row & 3))

    for k in range(4):
        other = mine ^ k
        if by_token:
            hidden[other] = pieces[k][...]
        else:
            hidden[:, :, pl.ds(pl.multiple_of(other * 512, 512), 512)] = pieces[k][...]
    for c in small:
        c.wait()
    kept[...] = hidden[mine]
    if by_token:
        half[...] = jnp.where((mine & 1) == 0, hidden[:, :, : D // 2], hidden[:, :, D // 2 :])
    wide = hidden[...].astype(jnp.float32).reshape(TOKENS, D)
    factor = lax.rsqrt(jnp.mean(wide * wide, axis=-1, keepdims=True) + EPS)
    normed = (wide * factor * gain[...]).astype(jnp.bfloat16)
    q = jnp.zeros((TOKENS, QH * HD), jnp.float32)
    new = jnp.zeros((TOKENS, KH * 2 * HD), jnp.float32)
    for p in range(chunks):
        at = pl.ds(p * step, step)
        arrived(p)
        part = normed[:, p * step : (p + 1) * step]
        q = q + jnp.dot(part, wq[at], preferred_element_type=jnp.float32)
        new = new + jnp.dot(part, wkv[at], preferred_element_type=jnp.float32)

    lane = lax.broadcasted_iota(jnp.int32, (TOKENS, 128), 1)
    low = (lane & 63) < 32
    left = lane < HD
    cos_all = cosine[...]
    sin_all = sine[...]

    def turned(block, c, s):
        other = jnp.where(low, pltpu.roll(block, 96, 1), pltpu.roll(block, 32, 1))
        return block * c + other * s

    scale = HD ** (-0.5)
    for m in range(QH // 2):
        block = turned(q[:, m * 128 : (m + 1) * 128], cos_all, sin_all) * scale
        pair = (jnp.where(left, block, 0.0), jnp.where(left, pltpu.roll(block, HD, 1), 0.0))
        for half in range(2):
            for j in range(DRAFT):
                at = ((2 * m + half) * DRAFT + j) * ROWS
                qs[at : at + ROWS, :] = pair[half][j * ROWS : (j + 1) * ROWS, :]
    key_cos = jnp.where(left, cos_all, 1.0)
    key_sin = jnp.where(left, sin_all, 0.0)
    for h in range(KH):
        block = turned(new[:, h * 128 : (h + 1) * 128], key_cos, key_sin)
        for i in range(DRAFT):
            at = (i * KH + h) * ROWS
            nk[at : at + ROWS, :] = block[i * ROWS : (i + 1) * ROWS, :]

    last = (((1,), (1,)), ((), ()))
    for r in range(ROWS):
        fresh = nk[pl.ds(r, DRAFT * KH, stride=ROWS), :].astype(jnp.bfloat16)
        asked = qs[pl.ds(r, 4 * QH, stride=ROWS), :].astype(jnp.bfloat16)
        if r % 2 == 0:
            arrived(chunks + r // 2)
        stored = kv[r]
        scores = lax.dot_general(asked, stored, last, preferred_element_type=jnp.float32)
        scores = jnp.where(slot[...] < KH * lens[r], scores, NEGATIVE)
        new_scores = lax.dot_general(asked, fresh, last, preferred_element_type=jnp.float32)
        new_scores = jnp.where(seen, new_scores, NEGATIVE)
        top = jnp.maximum(
            jnp.max(scores, axis=-1, keepdims=True), jnp.max(new_scores, axis=-1, keepdims=True)
        )
        weights = jnp.exp(scores - top)
        new_weights = jnp.exp(new_scores - top)
        total = jnp.sum(weights, axis=-1, keepdims=True) + jnp.sum(
            new_weights, axis=-1, keepdims=True
        )
        mixed = jnp.dot(
            weights.astype(jnp.bfloat16), stored, preferred_element_type=jnp.float32
        ) + jnp.dot(new_weights.astype(jnp.bfloat16), fresh, preferred_element_type=jnp.float32)
        hs[pl.ds(r, 4 * QH, stride=ROWS), :] = mixed / total

    side = lax.broadcasted_iota(jnp.int32, (ROWS, 128), 1) < HD
    rows = []
    for j in range(DRAFT):
        tiles = []
        for m in range(QH // 2):
            first = ((2 * m) * DRAFT + j) * ROWS
            second = ((2 * m + 1) * DRAFT + j) * ROWS
            tiles.append(
                jnp.where(
                    side, pltpu.roll(hs[first : first + ROWS, :], HD, 1), hs[second : second + ROWS, :]
                )
            )
        rows.append(jnp.concatenate(tiles, axis=1))
    heads = jnp.concatenate(rows, axis=0).astype(jnp.bfloat16)
    for p in range(4):
        arrived(chunks + ROWS // 2 + p)
    shares = jnp.dot(heads, wo[...], preferred_element_type=jnp.float32)
    for j in range(DRAFT):
        result[j] = shares[j * ROWS : (j + 1) * ROWS, :].astype(jnp.bfloat16)
    for k in range(4):
        out[k][...] = result[mine ^ k]


def attend(by_token, lens, me, pieces, gain, cosine, sine, wq, wkv, wo, kv):
    hbm = pl.BlockSpec(memory_space=pltpu.HBM)
    vmem = pl.BlockSpec(memory_space=pltpu.VMEM)
    smem = pl.BlockSpec(memory_space=pltpu.SMEM)
    quarter = jax.ShapeDtypeStruct((ROWS, D), jnp.bfloat16)
    return pl.pallas_call(
        functools.partial(attend_kernel, by_token),
        out_shape=[quarter] * 5 + [jax.ShapeDtypeStruct((DRAFT, ROWS, D // 2), jnp.bfloat16)],
        in_specs=[smem] * 2 + [vmem] * 4 + [hbm] * 7,
        out_specs=[vmem] * 6,
        scratch_shapes=[
            pltpu.VMEM((DRAFT, ROWS, D), jnp.bfloat16),
            pltpu.VMEM((1, D), jnp.float32),
            pltpu.VMEM((TOKENS, 128), jnp.float32),
            pltpu.VMEM((TOKENS, 128), jnp.float32),
            pltpu.VMEM((D, QH * HD), jnp.bfloat16),
            pltpu.VMEM((D, KH * 2 * HD), jnp.bfloat16),
            pltpu.VMEM((QH * HD, D), jnp.bfloat16),
            pltpu.VMEM((ROWS, SLOTS, 128), jnp.bfloat16),
            pltpu.VMEM((4 * QH * ROWS, 128), jnp.float32),
            pltpu.VMEM((DRAFT * KH * ROWS, 128), jnp.float32),
            pltpu.VMEM((4 * QH * ROWS, 128), jnp.float32),
            pltpu.VMEM((4 * QH, SLOTS), jnp.int32),
            pltpu.VMEM((DRAFT, ROWS, D), jnp.bfloat16),
            pltpu.SemaphoreType.DMA((35,)),
        ],
        compiler_params=pltpu.CompilerParams(vmem_limit_bytes=VMEM_LIMIT),
        cost_estimate=pl.CostEstimate(flops=400_000_000, transcendentals=800_000, bytes_accessed=13_500_000),
        name="attend",
    )(lens, me, *pieces, gain, cosine, sine, wq, wkv, wo, kv)


def mlp_kernel(halves, tokens, gathered, out, weights, sems):
    parts = gathered.shape[3]
    copies = [
        pltpu.make_async_copy(
            gathered.at[h, z, :, part],
            weights.at[z, :, h, :, pl.ds(part * FFS, FFS)],
            sems.at[(2 * z + h) * parts + part],
        )
        for z in range(Z)
        for h in range(2)
        for part in range(parts)
    ]
    for c in copies:
        c.start()
    count = tokens.shape[0]
    units = weights.shape[-1]
    gate = jnp.zeros((count, units), jnp.float32)
    up = jnp.zeros((count, units), jnp.float32)
    for z in range(Z):
        for c in copies[2 * z * parts : 2 * (z + 1) * parts]:
            c.wait()
        part = tokens[:, z * 256 : (z + 1) * 256]
        gate = gate + jnp.dot(
            part, weights[z, :, :, 0:16, :].reshape(256, units), preferred_element_type=jnp.float32
        )
        up = up + jnp.dot(
            part, weights[z, :, :, 16:32, :].reshape(256, units), preferred_element_type=jnp.float32
        )
    act = (gate / (1.0 + jnp.exp(-gate)) * up).astype(jnp.bfloat16)
    for z in range(Z):
        down = weights[z, :, :, 32:48, :].reshape(256, units)
        share = lax.dot_general(
            act, down, (((1,), (1,)), ((), ())), preferred_element_type=jnp.float32
        ).astype(jnp.bfloat16)
        if halves:
            share = share.reshape(2, count // (2 * ROWS), ROWS, 256)
            at = (z % 4) * 256
            for side in range(2):
                out[z // 4, :, side, :, at : at + 256] = share[side]
        else:
            out[:, z * 256 : (z + 1) * 256] = share


def mlp(tokens, gathered, halves):
    hbm = pl.BlockSpec(memory_space=pltpu.HBM)
    vmem = pl.BlockSpec(memory_space=pltpu.VMEM)
    units = gathered.shape[3] * FFS
    return pl.pallas_call(
        functools.partial(mlp_kernel, halves),
        out_shape=jax.ShapeDtypeStruct(
            (2, tokens.shape[0] // (2 * ROWS), 2, ROWS, D // 2) if halves else tokens.shape,
            jnp.bfloat16,
        ),
        in_specs=[vmem, hbm],
        out_specs=vmem,
        scratch_shapes=[
            pltpu.VMEM((Z, 8, 2, 48, units), jnp.bfloat16),
            pltpu.SemaphoreType.DMA((2 * Z * gathered.shape[3],)),
        ],
        compiler_params=pltpu.CompilerParams(vmem_limit_bytes=VMEM_LIMIT),
        cost_estimate=pl.CostEstimate(flops=400_000_000, transcendentals=32768, bytes_accessed=4_200_000),
        name="mlp",
    )(tokens, gathered)


def halves_kernel(section, gate, up, down, keep, give):
    for out, which in ((keep, section[0]), (give, 1 - section[0])):
        at = pl.ds(pl.multiple_of(which * 16, 16), 16)
        for g, w in enumerate((gate, up, down)):
            for a in range(8):
                out[a, g * 16 : (g + 1) * 16, :] = w[at, a * FFS : (a + 1) * FFS]


def laid_halves(section, gate, up, down):
    vmem = pl.BlockSpec(memory_space=pltpu.VMEM)
    return pl.pallas_call(
        halves_kernel,
        out_shape=[jax.ShapeDtypeStruct((8, 48, FFS), jnp.bfloat16)] * 2,
        in_specs=[pl.BlockSpec(memory_space=pltpu.SMEM), vmem, vmem, vmem],
        out_specs=[vmem, vmem],
        compiler_params=pltpu.CompilerParams(vmem_limit_bytes=VMEM_LIMIT),
        name="halves",
    )(section, gate, up, down)


def after(first, then):
    return lax.optimization_barrier((first, then))[1]


def exchanged(blocks):
    return [
        lax.ppermute(blocks[k], CHIP, [(i, i ^ k) for i in range(4)]) for k in (1, 2, 3)
    ]


def normalize(hidden, gain):
    wide = hidden.astype(jnp.float32)
    factor = lax.rsqrt(jnp.mean(wide * wide, axis=-1, keepdims=True) + EPS)
    return (wide * factor * gain).astype(jnp.bfloat16)


def local(
    exit_hidden,
    exit_depth,
    context_len,
    attn_gain,
    w_query,
    w_keyval,
    w_out,
    kv_cache,
    mlp_gain,
    w_gate,
    w_up,
    w_down,
):
    section = lax.axis_index("section")
    tensor = lax.axis_index("tensor")

    kept_half, sent_half = laid_halves(section.reshape(1), w_gate[0], w_up[0], w_down[0])
    got_half = lax.ppermute(sent_half, "section", [(0, 1), (1, 0)])
    first = jnp.where(section == 0, kept_half, got_half)
    second = jnp.where(section == 1, kept_half, got_half)
    block0 = lax.all_to_all(first, ("y", "xh"), 0, 0, tiled=True)

    other_gain = lax.ppermute(mlp_gain, "section", [(0, 1), (1, 0)])
    gains = [jnp.where(section == l, mlp_gain, other_gain) for l in range(2)]
    own_piece = exit_hidden.transpose(1, 0, 2)
    pieces = [own_piece] + exchanged([own_piece] * 4)

    def gathered(block):
        g = lax.all_gather(block, ("section", "z"), axis=0)
        return g.reshape(2, Z, 8, -1, 48, FFS)

    weights = [gathered(after((pieces, other_gain), block0))]
    slices = jnp.broadcast_to(
        second.reshape(4, 1, 2, 48, FFS), (4, 2, 2, 48, FFS)
    ).reshape(8, 2, 48, FFS)
    block1 = lax.all_to_all(after(pieces[3], slices), ("y", "xh"), 0, 0, tiled=True)

    where_at = (jnp.arange(DRAFT, dtype=jnp.int32)[:, None] + context_len[None, :]).reshape(TOKENS)
    rates = jnp.exp(jnp.arange(HD // 2, dtype=jnp.float32) * (-2.0 * math.log(THETA) / HD))
    angles = where_at.astype(jnp.float32)[:, None] * rates
    c = jnp.cos(angles)
    s = jnp.sin(angles)
    cosine = jnp.concatenate([c, c, c, c], axis=1)
    sine = jnp.concatenate([-s, s, -s, s], axis=1)

    cache = kv_cache[0].reshape(ROWS, SLOTS, 128)
    me = section * 2 + tensor
    for l in range(2):
        *partial, before, half = attend(
            l == 1,
            context_len,
            me.reshape(1),
            pieces,
            attn_gain,
            cosine,
            sine,
            w_query[0],
            w_keyval[0],
            w_out[0],
            cache,
        )
        near, across, far = exchanged(partial)
        mine = section == l
        mid = (
            before.astype(jnp.float32)
            + jnp.where(mine, partial[0], across).astype(jnp.float32)
            + jnp.where(mine, near, far).astype(jnp.float32)
        ).astype(jnp.bfloat16)
        if l == 0:
            weights.append(gathered(after(mid, block1)))
        mlp_in = normalize(mid, gains[l])
        axes, group = GROUPS[l]
        everyone = lax.all_to_all(
            jnp.broadcast_to(mlp_in[None], (group, ROWS, D)), axes, 0, 0, tiled=True
        )
        share = mlp(everyone.reshape(group * ROWS, D), weights[l], l == 1)
        if l == 0:
            shares = lax.all_to_all(share.reshape(group, ROWS, D), axes, 0, 0, tiled=True)
            total = jnp.sum(shares.astype(jnp.float32), axis=0)
            updated = (mid.astype(jnp.float32) + total).astype(jnp.bfloat16)
            kept = jnp.where((exit_depth <= l)[:, None], updated, before)
            pieces = [kept] + exchanged([kept] * 4)
    left, right = mid[:, : D // 2], mid[:, D // 2 :]
    same = jnp.where(tensor == 0, left, right)
    opposite = jnp.where(tensor == 0, right, left)
    got = lax.ppermute(opposite, "tensor", [(0, 1), (1, 0)])
    mids = jnp.where(tensor == 0, jnp.stack([same, got]), jnp.stack([got, same]))
    shares = lax.all_to_all(share.reshape(8, 2, ROWS, D // 2), axes, 0, 0, tiled=True)
    total = jnp.sum(shares.astype(jnp.float32), axis=0)
    updated = (mids.astype(jnp.float32) + total).astype(jnp.bfloat16)
    sent = lax.ppermute(updated, "section", [(0, 1)])
    last = jnp.concatenate([sent, updated])
    return jnp.where(section == 0, half, last).transpose(1, 0, 2)[None]


def solution(mesh):
    wide = Mesh(mesh.devices.reshape(2, 2, Z, 4, 2), ("section", "tensor", "z", "y", "xh"))
    dp = ("z", "y", "xh")
    in_specs = (
        P(dp, None, ("section", "tensor")),
        P(dp),
        P(dp),
        P("section", None),
        P("section", None, "tensor"),
        P("section", None, "tensor"),
        P("section", "tensor", None),
        P("section", dp, None, "tensor", None),
        P("section", None),
        P("section", dp, "tensor"),
        P("section", dp, "tensor"),
        P("section", dp, "tensor"),
    )
    out_specs = P("section", dp, None, "tensor")

    return jax.shard_map(local, mesh=wide, in_specs=in_specs, out_specs=out_specs, check_vma=False)
```

```python
import functools
import math

import jax
import jax.numpy as jnp
from jax import lax
from jax.experimental import pallas as pl
from jax.experimental.pallas import tpu as pltpu
from jax.sharding import Mesh, PartitionSpec as P


D = 2048
DRAFT = 4
CTX = 384
ROWS = 8
TOKENS = ROWS * DRAFT
HD = 64
QH = 16
KH = 4
SLOTS = CTX * KH
VMEM_LIMIT = 53000 * 1024
AHEAD = 8
FFS = 256
EPS = 1e-05
THETA = 500000.0
NEGATIVE = -1e30
GROUPS = ((("tensor", "y", "xh"), 16), (("tensor", "y"), 8))
CHIP = ("section", "tensor")
Z = 8


def attend_kernel(
    by_token, lens, me, *refs
):
    pieces, refs = refs[:4], refs[4:]
    gain_h, cos_h, sin_h, wq_h, wkv_h, wo_h, kv_h, *refs = refs
    out, refs = refs[:4], refs[4:]
    kept, half, *refs = refs
    hidden, gain, cosine, sine, wq, wkv, wo, kv, qs, nk, hs, slot, result, sems = refs
    mine = me[0]
    small = []
    small.append(pltpu.make_async_copy(gain_h, gain, sems.at[4]))
    small.append(pltpu.make_async_copy(cos_h, cosine, sems.at[5]))
    small.append(pltpu.make_async_copy(sin_h, sine, sems.at[6]))
    chunks = 8
    step = D // chunks
    copies = []
    for p in range(chunks):
        at = pl.ds(p * step, step)
        copies.append(pltpu.make_async_copy(wq_h.at[at], wq.at[at], sems.at[7 + 2 * p]))
        copies.append(pltpu.make_async_copy(wkv_h.at[at], wkv.at[at], sems.at[8 + 2 * p]))
    base = 7 + 2 * chunks
    kv_copies = [
        pltpu.make_async_copy(kv_h.at[r], kv.at[r], sems.at[base + r]) for r in range(ROWS)
    ]
    wo_copies = [
        pltpu.make_async_copy(
            wo_h.at[pl.ds(p * 256, 256)], wo.at[pl.ds(p * 256, 256)], sems.at[base + ROWS + p]
        )
        for p in range(4)
    ]
    queue = [copies[2 * p : 2 * p + 2] for p in range(chunks)] + [
        kv_copies[2 * p : 2 * p + 2] for p in range(ROWS // 2)
    ]
    queue += [[c] for c in wo_copies]
    for c in small:
        c.start()
    for group in queue[:AHEAD]:
        for c in group:
            c.start()

    def arrived(n):
        for c in queue[n]:
            c.wait()
        if n + AHEAD < len(queue):
            for c in queue[n + AHEAD]:
                c.start()

    row = lax.broadcasted_iota(jnp.int32, (4 * QH, SLOTS), 0)
    place = lax.broadcasted_iota(jnp.int32, (4 * QH, SLOTS), 1)
    slot[...] = jnp.where((place & 3) == (row >> 4), place, SLOTS)
    new_row = lax.broadcasted_iota(jnp.int32, (4 * QH, DRAFT * KH), 0)
    new_col = lax.broadcasted_iota(jnp.int32, (4 * QH, DRAFT * KH), 1)
    seen = ((new_col & 3) == (new_row >> 4)) & ((new_col >> 2) <= (new_row & 3))

    for k in range(4):
        other = mine ^ k
        if by_token:
            hidden[other] = pieces[k][...]
        else:
            hidden[:, :, pl.ds(pl.multiple_of(other * 512, 512), 512)] = pieces[k][...]
    for c in small:
        c.wait()
    kept[...] = hidden[mine]
    if by_token:
        half[...] = jnp.where((mine & 1) == 0, hidden[:, :, : D // 2], hidden[:, :, D // 2 :])
    wide = hidden[...].astype(jnp.float32).reshape(TOKENS, D)
    factor = lax.rsqrt(jnp.mean(wide * wide, axis=-1, keepdims=True) + EPS)
    normed = (wide * factor * gain[...]).astype(jnp.bfloat16)
    q = jnp.zeros((TOKENS, QH * HD), jnp.float32)
    new = jnp.zeros((TOKENS, KH * 2 * HD), jnp.float32)
    for p in range(chunks):
        at = pl.ds(p * step, step)
        arrived(p)
        part = normed[:, p * step : (p + 1) * step]
        q = q + jnp.dot(part, wq[at], preferred_element_type=jnp.float32)
        new = new + jnp.dot(part, wkv[at], preferred_element_type=jnp.float32)

    lane = lax.broadcasted_iota(jnp.int32, (TOKENS, 128), 1)
    low = (lane & 63) < 32
    left = lane < HD
    cos_all = cosine[...]
    sin_all = sine[...]

    def turned(block, c, s):
        other = jnp.where(low, pltpu.roll(block, 96, 1), pltpu.roll(block, 32, 1))
        return block * c + other * s

    scale = HD ** (-0.5)
    for m in range(QH // 2):
        block = turned(q[:, m * 128 : (m + 1) * 128], cos_all, sin_all) * scale
        pair = (jnp.where(left, block, 0.0), jnp.where(left, pltpu.roll(block, HD, 1), 0.0))
        for half in range(2):
            for j in range(DRAFT):
                at = ((2 * m + half) * DRAFT + j) * ROWS
                qs[at : at + ROWS, :] = pair[half][j * ROWS : (j + 1) * ROWS, :]
    key_cos = jnp.where(left, cos_all, 1.0)
    key_sin = jnp.where(left, sin_all, 0.0)
    for h in range(KH):
        block = turned(new[:, h * 128 : (h + 1) * 128], key_cos, key_sin)
        for i in range(DRAFT):
            at = (i * KH + h) * ROWS
            nk[at : at + ROWS, :] = block[i * ROWS : (i + 1) * ROWS, :]

    last = (((1,), (1,)), ((), ()))
    for r in range(ROWS):
        fresh = nk[pl.ds(r, DRAFT * KH, stride=ROWS), :].astype(jnp.bfloat16)
        asked = qs[pl.ds(r, 4 * QH, stride=ROWS), :].astype(jnp.bfloat16)
        if r % 2 == 0:
            arrived(chunks + r // 2)
        stored = kv[r]
        scores = lax.dot_general(asked, stored, last, preferred_element_type=jnp.float32)
        scores = jnp.where(slot[...] < KH * lens[r], scores, NEGATIVE)
        new_scores = lax.dot_general(asked, fresh, last, preferred_element_type=jnp.float32)
        new_scores = jnp.where(seen, new_scores, NEGATIVE)
        top = jnp.maximum(
            jnp.max(scores, axis=-1, keepdims=True), jnp.max(new_scores, axis=-1, keepdims=True)
        )
        weights = jnp.exp(scores - top)
        new_weights = jnp.exp(new_scores - top)
        total = jnp.sum(weights, axis=-1, keepdims=True) + jnp.sum(
            new_weights, axis=-1, keepdims=True
        )
        mixed = jnp.dot(
            weights.astype(jnp.bfloat16), stored, preferred_element_type=jnp.float32
        ) + jnp.dot(new_weights.astype(jnp.bfloat16), fresh, preferred_element_type=jnp.float32)
        hs[pl.ds(r, 4 * QH, stride=ROWS), :] = mixed / total

    side = lax.broadcasted_iota(jnp.int32, (ROWS, 128), 1) < HD
    rows = []
    for j in range(DRAFT):
        tiles = []
        for m in range(QH // 2):
            first = ((2 * m) * DRAFT + j) * ROWS
            second = ((2 * m + 1) * DRAFT + j) * ROWS
            tiles.append(
                jnp.where(
                    side, pltpu.roll(hs[first : first + ROWS, :], HD, 1), hs[second : second + ROWS, :]
                )
            )
        rows.append(jnp.concatenate(tiles, axis=1))
    heads = jnp.concatenate(rows, axis=0).astype(jnp.bfloat16)
    for p in range(4):
        arrived(chunks + ROWS // 2 + p)
    shares = jnp.dot(heads, wo[...], preferred_element_type=jnp.float32)
    for j in range(DRAFT):
        result[j] = shares[j * ROWS : (j + 1) * ROWS, :].astype(jnp.bfloat16)
    for k in range(4):
        out[k][...] = result[mine ^ k]


def attend(by_token, lens, me, pieces, gain, cosine, sine, wq, wkv, wo, kv):
    hbm = pl.BlockSpec(memory_space=pltpu.HBM)
    vmem = pl.BlockSpec(memory_space=pltpu.VMEM)
    smem = pl.BlockSpec(memory_space=pltpu.SMEM)
    quarter = jax.ShapeDtypeStruct((ROWS, D), jnp.bfloat16)
    return pl.pallas_call(
        functools.partial(attend_kernel, by_token),
        out_shape=[quarter] * 5 + [jax.ShapeDtypeStruct((DRAFT, ROWS, D // 2), jnp.bfloat16)],
        in_specs=[smem] * 2 + [vmem] * 4 + [hbm] * 7,
        out_specs=[vmem] * 6,
        scratch_shapes=[
            pltpu.VMEM((DRAFT, ROWS, D), jnp.bfloat16),
            pltpu.VMEM((1, D), jnp.float32),
            pltpu.VMEM((TOKENS, 128), jnp.float32),
            pltpu.VMEM((TOKENS, 128), jnp.float32),
            pltpu.VMEM((D, QH * HD), jnp.bfloat16),
            pltpu.VMEM((D, KH * 2 * HD), jnp.bfloat16),
            pltpu.VMEM((QH * HD, D), jnp.bfloat16),
            pltpu.VMEM((ROWS, SLOTS, 128), jnp.bfloat16),
            pltpu.VMEM((4 * QH * ROWS, 128), jnp.float32),
            pltpu.VMEM((DRAFT * KH * ROWS, 128), jnp.float32),
            pltpu.VMEM((4 * QH * ROWS, 128), jnp.float32),
            pltpu.VMEM((4 * QH, SLOTS), jnp.int32),
            pltpu.VMEM((DRAFT, ROWS, D), jnp.bfloat16),
            pltpu.SemaphoreType.DMA((35,)),
        ],
        compiler_params=pltpu.CompilerParams(vmem_limit_bytes=VMEM_LIMIT),
        cost_estimate=pl.CostEstimate(flops=400_000_000, transcendentals=800_000, bytes_accessed=13_500_000),
        name="attend",
    )(lens, me, *pieces, gain, cosine, sine, wq, wkv, wo, kv)


def mlp_kernel(halves, tokens, gathered, out, weights, sems):
    parts = gathered.shape[3]
    copies = [
        pltpu.make_async_copy(
            gathered.at[h, z, :, part],
            weights.at[z, :, h, :, pl.ds(part * FFS, FFS)],
            sems.at[(2 * z + h) * parts + part],
        )
        for z in range(Z)
        for h in range(2)
        for part in range(parts)
    ]
    for c in copies:
        c.start()
    count = tokens.shape[0]
    units = weights.shape[-1]
    gate = jnp.zeros((count, units), jnp.float32)
    up = jnp.zeros((count, units), jnp.float32)
    for z in range(Z):
        for c in copies[2 * z * parts : 2 * (z + 1) * parts]:
            c.wait()
        part = tokens[:, z * 256 : (z + 1) * 256]
        gate = gate + jnp.dot(
            part, weights[z, :, :, 0:16, :].reshape(256, units), preferred_element_type=jnp.float32
        )
        up = up + jnp.dot(
            part, weights[z, :, :, 16:32, :].reshape(256, units), preferred_element_type=jnp.float32
        )
    act = (gate / (1.0 + jnp.exp(-gate)) * up).astype(jnp.bfloat16)
    for z in range(Z):
        down = weights[z, :, :, 32:48, :].reshape(256, units)
        share = lax.dot_general(
            act, down, (((1,), (1,)), ((), ())), preferred_element_type=jnp.float32
        ).astype(jnp.bfloat16)
        if halves:
            share = share.reshape(2, count // (2 * ROWS), ROWS, 256)
            at = (z % 4) * 256
            for side in range(2):
                out[z // 4, :, side, :, at : at + 256] = share[side]
        else:
            out[:, z * 256 : (z + 1) * 256] = share


def mlp(tokens, gathered, halves):
    hbm = pl.BlockSpec(memory_space=pltpu.HBM)
    vmem = pl.BlockSpec(memory_space=pltpu.VMEM)
    units = gathered.shape[3] * FFS
    return pl.pallas_call(
        functools.partial(mlp_kernel, halves),
        out_shape=jax.ShapeDtypeStruct(
            (2, tokens.shape[0] // (2 * ROWS), 2, ROWS, D // 2) if halves else tokens.shape,
            jnp.bfloat16,
        ),
        in_specs=[vmem, hbm],
        out_specs=vmem,
        scratch_shapes=[
            pltpu.VMEM((Z, 8, 2, 48, units), jnp.bfloat16),
            pltpu.SemaphoreType.DMA((2 * Z * gathered.shape[3],)),
        ],
        compiler_params=pltpu.CompilerParams(vmem_limit_bytes=VMEM_LIMIT),
        cost_estimate=pl.CostEstimate(flops=400_000_000, transcendentals=32768, bytes_accessed=4_200_000),
        name="mlp",
    )(tokens, gathered)


def halves_kernel(section, gate_h, up_h, down_h, keep, give, gate, up, down, sems):
    copies = [
        pltpu.make_async_copy(h, v, sems.at[n])
        for n, (h, v) in enumerate(((gate_h, gate), (up_h, up), (down_h, down)))
    ]
    for c in copies:
        c.start()
    for c in copies:
        c.wait()
    for out, which in ((keep, section[0]), (give, 1 - section[0])):
        at = pl.ds(pl.multiple_of(which * 16, 16), 16)
        for g, w in enumerate((gate, up, down)):
            for a in range(8):
                out[a, g * 16 : (g + 1) * 16, :] = w[at, a * FFS : (a + 1) * FFS]


def laid_halves(section, gate, up, down):
    vmem = pl.BlockSpec(memory_space=pltpu.VMEM)
    return pl.pallas_call(
        halves_kernel,
        out_shape=[jax.ShapeDtypeStruct((8, 48, FFS), jnp.bfloat16)] * 2,
        in_specs=[pl.BlockSpec(memory_space=pltpu.SMEM)]
        + [pl.BlockSpec(memory_space=pltpu.HBM)] * 3,
        out_specs=[vmem, vmem],
        scratch_shapes=[pltpu.VMEM((32, D), jnp.bfloat16)] * 3 + [pltpu.SemaphoreType.DMA((3,))],
        compiler_params=pltpu.CompilerParams(vmem_limit_bytes=60 * 1024 * 1024),
        name="halves",
    )(section, gate, up, down)


def after(first, then):
    return lax.optimization_barrier((first, then))[1]


def exchanged(blocks):
    return [
        lax.ppermute(blocks[k], CHIP, [(i, i ^ k) for i in range(4)]) for k in (1, 2, 3)
    ]


def normalize(hidden, gain):
    wide = hidden.astype(jnp.float32)
    factor = lax.rsqrt(jnp.mean(wide * wide, axis=-1, keepdims=True) + EPS)
    return (wide * factor * gain).astype(jnp.bfloat16)


def local(
    exit_hidden,
    exit_depth,
    context_len,
    attn_gain,
    w_query,
    w_keyval,
    w_out,
    kv_cache,
    mlp_gain,
    w_gate,
    w_up,
    w_down,
):
    section = lax.axis_index("section")
    tensor = lax.axis_index("tensor")

    kept_half, sent_half = laid_halves(section.reshape(1), w_gate[0], w_up[0], w_down[0])
    got_half = lax.ppermute(sent_half, "section", [(0, 1), (1, 0)])
    first = jnp.where(section == 0, kept_half, got_half)
    second = jnp.where(section == 1, kept_half, got_half)
    block0 = lax.all_to_all(first, ("y", "xh"), 0, 0, tiled=True)

    other_gain = lax.ppermute(mlp_gain, "section", [(0, 1), (1, 0)])
    gains = [jnp.where(section == l, mlp_gain, other_gain) for l in range(2)]
    own_piece = exit_hidden.transpose(1, 0, 2)
    pieces = [own_piece] + exchanged([own_piece] * 4)

    def gathered(block):
        g = lax.all_gather(block, ("section", "z"), axis=0)
        return g.reshape(2, Z, 8, -1, 48, FFS)

    weights = [gathered(after((pieces, other_gain), block0))]
    slices = jnp.broadcast_to(
        second.reshape(4, 1, 2, 48, FFS), (4, 2, 2, 48, FFS)
    ).reshape(8, 2, 48, FFS)
    block1 = lax.all_to_all(after(pieces[3], slices), ("y", "xh"), 0, 0, tiled=True)

    where_at = (jnp.arange(DRAFT, dtype=jnp.int32)[:, None] + context_len[None, :]).reshape(TOKENS)
    rates = jnp.exp(jnp.arange(HD // 2, dtype=jnp.float32) * (-2.0 * math.log(THETA) / HD))
    angles = where_at.astype(jnp.float32)[:, None] * rates
    c = jnp.cos(angles)
    s = jnp.sin(angles)
    cosine = jnp.concatenate([c, c, c, c], axis=1)
    sine = jnp.concatenate([-s, s, -s, s], axis=1)

    cache = kv_cache[0].reshape(ROWS, SLOTS, 128)
    me = section * 2 + tensor
    for l in range(2):
        *partial, before, half = attend(
            l == 1,
            context_len,
            me.reshape(1),
            pieces,
            attn_gain,
            cosine,
            sine,
            w_query[0],
            w_keyval[0],
            w_out[0],
            cache,
        )
        near, across, far = exchanged(partial)
        mine = section == l
        mid = (
            before.astype(jnp.float32)
            + jnp.where(mine, partial[0], across).astype(jnp.float32)
            + jnp.where(mine, near, far).astype(jnp.float32)
        ).astype(jnp.bfloat16)
        if l == 0:
            weights.append(gathered(after(mid, block1)))
        mlp_in = normalize(mid, gains[l])
        axes, group = GROUPS[l]
        everyone = lax.all_to_all(
            jnp.broadcast_to(mlp_in[None], (group, ROWS, D)), axes, 0, 0, tiled=True
        )
        share = mlp(everyone.reshape(group * ROWS, D), weights[l], l == 1)
        if l == 0:
            shares = lax.all_to_all(share.reshape(group, ROWS, D), axes, 0, 0, tiled=True)
            total = jnp.sum(shares.astype(jnp.float32), axis=0)
            updated = (mid.astype(jnp.float32) + total).astype(jnp.bfloat16)
            kept = jnp.where((exit_depth <= l)[:, None], updated, before)
            pieces = [kept] + exchanged([kept] * 4)
    left, right = mid[:, : D // 2], mid[:, D // 2 :]
    same = jnp.where(tensor == 0, left, right)
    opposite = jnp.where(tensor == 0, right, left)
    got = lax.ppermute(opposite, "tensor", [(0, 1), (1, 0)])
    mids = jnp.where(tensor == 0, jnp.stack([same, got]), jnp.stack([got, same]))
    shares = lax.all_to_all(share.reshape(8, 2, ROWS, D // 2), axes, 0, 0, tiled=True)
    total = jnp.sum(shares.astype(jnp.float32), axis=0)
    updated = (mids.astype(jnp.float32) + total).astype(jnp.bfloat16)
    sent = lax.ppermute(updated, "section", [(0, 1)])
    last = jnp.concatenate([sent, updated])
    return jnp.where(section == 0, half, last).transpose(1, 0, 2)[None]


def solution(mesh):
    wide = Mesh(mesh.devices.reshape(2, 2, Z, 4, 2), ("section", "tensor", "z", "y", "xh"))
    dp = ("z", "y", "xh")
    in_specs = (
        P(dp, None, ("section", "tensor")),
        P(dp),
        P(dp),
        P("section", None),
        P("section", None, "tensor"),
        P("section", None, "tensor"),
        P("section", "tensor", None),
        P("section", dp, None, "tensor", None),
        P("section", None),
        P("section", dp, "tensor"),
        P("section", dp, "tensor"),
        P("section", dp, "tensor"),
    )
    out_specs = P("section", dp, None, "tensor")

    return jax.shard_map(local, mesh=wide, in_specs=in_specs, out_specs=out_specs, check_vma=False)
```
